128 devices in a mesh: grp: 2 (over x_lo), dev: 64 (over x_hi, z, y, core).
Axes of the slice: x: 4 (x_hi: 2, x_lo: 2; x = x_hi * 2 + x_lo), y: 4, z: 4, core: 2. Of those that a mesh axis runs over, the one named last changes fastest.
Arguments:
- frames: float32 [2, 128, 512, 512], P('grp', 'dev'), may hold values from -6 to 6
- ref_spectrum: float32 [2, 128, 512, 512], P(None, None, 'dev'), as said below
- shifts: int32 [2, 3], replicated, may hold values from 0 to 127
- offsets: int32 [2, 3], replicated, may hold values from 0 to 127
Outputs:
- correlation: float32 [2, 128, 128, 128], P('grp', 'dev')
- new_reference: float32 [2, 128, 512, 512], P(None, 'grp', 'dev')
The draws below stay inside these ranges and needn't reach their ends.
Inputs may be any that keep to these rules, and one draw needn't show every extreme that they name: `ref_spectrum`: real and imaginary parts are real numbers.
All inputs are finite; a program needn't handle non-finite values.
Results may differ from the reference program's by a relative error of at most 0.0001.
Values sent between devices are 32-bit elements; how exact they have to be, the bound alone decides.
A program may use at most 128 MiB of HBM per device.

```python
import math
import jax
import jax.numpy as jnp

NX = 512
NY = 512
NZ = 128
CROP = 128
TIMES = 2


def draw_ref_spectrum(key, part):
    first, second = jax.random.split(key)
    base = jax.random.normal(first, (2, NZ, NY, NX), jnp.float32)
    spread = 10.0
    rows = jnp.arange(NY, dtype=jnp.float32) / (NY - 1)
    row_scale = spread ** (rows - 0.5)
    column_scale = jnp.exp(jax.random.uniform(second, (NX,), jnp.float32, 0.0, math.log(3.0)))
    return base * row_scale[None, None, :, None] * column_scale[None, None, None, :]


def with_ends(result, stream_key, low, top_value):
    longest = result.shape.index(max(result.shape))
    spots = []
    for shift in (0, 1):
        where = [jax.random.randint(jax.random.fold_in(stream_key, axis), (), 0, length) for axis, length in enumerate(result.shape)]
        where[longest] = (where[longest] + shift) % result.shape[longest]
        spots.append(tuple(where))
    return result.at[spots[0]].set(low).at[spots[1]].set(top_value)


def levels(own_key, dims, shards, low, top_value):
    loudness, own = 1.0, jax.random.fold_in(own_key, 6)
    for position, shards_of in shards:
        steps = jnp.exp(jax.random.uniform(jax.random.fold_in(own, position), (shards_of,), jnp.float32, low / len(shards), top_value / len(shards)))
        loudness = loudness * jnp.repeat(steps, dims[position] // shards_of).reshape([-1 if axis == position else 1 for axis in range(len(dims))])
    return loudness


def normal_values(key, dims, scale, reach, shards=(), kind=jnp.bfloat16):
    loudness = levels(key, dims, shards, -0.22, 0.18) if shards else 1.0
    array = jax.random.normal(key, dims, jnp.float32) * scale * loudness
    return jnp.minimum(jnp.maximum(array, -reach), reach).astype(kind)


def setup_inputs(seed: int = 0) -> dict:
    arg_keys = jax.random.split(jax.random.key(seed), 5)
    return {
        "frames": normal_values(arg_keys[0], (TIMES, NZ, NY, NX), 1.0, 6.0, ((0, 2), (1, 64)), jnp.float32),
        "ref_spectrum": draw_ref_spectrum(jax.random.fold_in(arg_keys[4], 71), 0),
        "shifts": with_ends(jax.random.randint(arg_keys[2], (TIMES, 3), 0, NZ), jax.random.fold_in(arg_keys[2], 1), 0, NZ - 1).astype(jnp.int32),
        "offsets": with_ends(jax.random.randint(arg_keys[3], (TIMES, 3), 0, NZ), jax.random.fold_in(arg_keys[3], 1), 0, NZ - 1).astype(jnp.int32),
    }


def reference(frames, ref_spectrum, shifts, offsets):
    total = NZ * NY * NX
    root = math.sqrt(total)
    spectrum_ref = ref_spectrum[0] + 1j * ref_spectrum[1]
    results = []
    warped_sum = jnp.zeros_like(spectrum_ref)
    for timepoint in range(TIMES):
        frame = frames[timepoint]
        spectrum = jnp.fft.fftn(frame) / root
        cross = spectrum * jnp.conj(spectrum_ref)
        magnitude = jnp.abs(cross)
        average = jnp.sum(magnitude) / total
        whitened = cross / (magnitude + average)
        field = jnp.real(jnp.fft.ifftn(whitened)) * root
        offset = offsets[timepoint]
        index_z = ((offset[0] + jnp.arange(CROP, dtype=jnp.int32)) % NZ).astype(jnp.int32)
        index_y = ((offset[1] + jnp.arange(CROP, dtype=jnp.int32)) % NY).astype(jnp.int32)
        index_x = ((offset[2] + jnp.arange(CROP, dtype=jnp.int32)) % NX).astype(jnp.int32)
        cropped = jnp.take(field, index_z, axis=0)
        cropped = jnp.take(cropped, index_y, axis=1)
        cropped = jnp.take(cropped, index_x, axis=2)
        results.append(cropped.astype(jnp.float32))
        drift = shifts[timepoint]
        moved = jnp.roll(frame, (drift[0], drift[1], drift[2]), axis=(0, 1, 2))
        warped_sum = warped_sum + jnp.fft.fftn(moved) / root
    updated = 0.5 * spectrum_ref + 0.25 * warped_sum
    new_reference = jnp.stack([jnp.real(updated), jnp.imag(updated)]).astype(jnp.float32)
    return (jnp.stack(results), new_reference)
```

```python
import math

import jax
import jax.numpy as jnp
import numpy as np
from jax import lax
from jax.experimental import pallas as pl
from jax.experimental.pallas import tpu as pltpu
from jax.sharding import PartitionSpec as P

NX = 512
NY = 512
NZ = 128
CROP = 128
ROWS = 4
LANES = 128
BLOCKS = NX // LANES
WIDE = ROWS * LANES
DEVICES = 128
CHUNKS = 4
GROUPS = 16
SPAN = (GROUPS + 2) * 8
FACTOR = 1.0 / math.sqrt(NZ * NY * NX)
F32 = jnp.float32
BF16 = jnp.bfloat16
MESH = pl.DeviceIdType.MESH


def halves(table):
    single = table.astype(np.float32)
    high = single.astype(jnp.bfloat16)
    low = (table - high.astype(np.float64)).astype(np.float32).astype(jnp.bfloat16)
    return np.stack([high, low])


def forward_y_table():
    out = np.zeros((CHUNKS, GROUPS + 2, 2, ROWS, NY))
    y = np.arange(NY)
    for chunk in range(CHUNKS):
        for slot in range(GROUPS + 2):
            for j in range(ROWS):
                ky = 4 * (GROUPS * chunk + slot) + j
                angle = 2.0 * np.pi * (ky * y % NY) / NY
                out[chunk, slot, 0, j] = np.cos(angle)
                out[chunk, slot, 1, j] = -np.sin(angle)
    return halves(out.reshape(CHUNKS * SPAN, NY))


def forward_x_table():
    angle = 2.0 * np.pi * (np.arange(NX)[:, None] * np.arange(NX)[None, :] % NX) / NX
    return halves(np.concatenate([np.cos(angle), np.sin(angle)], axis=1))


def z_table(inverse):
    angle = 2.0 * np.pi * (np.arange(NZ)[:, None] * np.arange(NZ)[None, :] % NZ) / NZ
    c, s = np.cos(angle), np.sin(angle)
    if inverse:
        return halves(np.block([[c, -s], [s, c]]))
    return halves(FACTOR * np.block([[c, s], [-s, c]]))


def inverse_x_table():
    kx, x = np.arange(NX), np.arange(CROP)
    angle = 2.0 * np.pi * (kx[:, None] * x[None, :] % NX) / NX
    c, s = np.cos(angle), np.sin(angle)
    real = np.concatenate([c, s], axis=1).reshape(BLOCKS, LANES, 2 * CROP)
    imag = np.concatenate([-s, c], axis=1).reshape(BLOCKS, LANES, 2 * CROP)
    return halves(np.stack([real, imag], axis=1).reshape(2 * NX, 2 * CROP))


def inverse_y_table():
    group = np.arange(DEVICES)[:, None]
    j = np.arange(ROWS)[None, :]
    ky = 4 * group + np.where(group < DEVICES // 2, j, (4 - j) % 4)
    angle = 2.0 * np.pi * (np.arange(CROP)[:, None, None] * ky[None] % NY) / NY
    table = np.stack([np.cos(angle), -np.sin(angle)], axis=2)
    return halves(FACTOR * table.reshape(CROP, DEVICES * 8))


def split(a):
    high = a.astype(BF16)
    return high, (a - high.astype(F32)).astype(BF16)


def dot(a, b):
    return jnp.dot(a, b, preferred_element_type=F32)


def kernel(
    frames, dy, cs, zf, zi, xi, yi, shifts, offsets, ref_hbm,
    corr, nout,
    fhi, flo, sbuf, xbuf, rin, rbuf, cbuf, mbuf, nbuf, nrecv, ramp_xy, ramp_z,
    mine, abuf, g1hi, g1lo, gbuf, ybuf,
    send_x, recv_x, send_a, recv_a, send_n, recv_n, send_g, recv_g, ref_sem, own_sem,
):
    g = lax.axis_index("grp")
    d = lax.axis_index("dev")
    me = 2 * d + g
    core, y_at, z_at = d % 2, (d // 2) % 4, (d // 8) % 4
    upper = d // 32

    barrier = pltpu.get_barrier_semaphore()

    def greet(k, carry):
        to = (me + k) % DEVICES
        pl.semaphore_signal(barrier, 1, device_id=(to % 2, to // 2), device_id_type=MESH)
        return carry

    lax.fori_loop(1, DEVICES, greet, 0)
    for b in range(BLOCKS):
        pltpu.make_async_copy(ref_hbm.at[:, :, b * LANES : (b + 1) * LANES], rin.at[b], ref_sem).start()

    for p in range(2):
        high, low = split(frames[p])
        fhi[p] = high
        flo[p] = low

    sub = lax.broadcasted_iota(jnp.int32, (1, 8, NX), 1)
    sigma = jnp.where(sub < 4, 1.0, -1.0).astype(F32)
    first = (sub % 4) == 0

    def forward(i, carry):
        chunk = (z_at + i) % CHUNKS
        base = pl.multiple_of(chunk * SPAN, 16)
        dyh = dy[0, pl.ds(base, SPAN), :]
        dyl = dy[1, pl.ds(base, SPAN), :]
        for p in range(2):
            rows = dot(dyh, fhi[p]) + dot(dyh, flo[p]) + dot(dyl, fhi[p])
            rh, rl = split(rows)
            prod = dot(rh, cs[0]) + dot(rl, cs[0]) + dot(rh, cs[1])
            prod = prod.reshape(GROUPS + 2, 8, 2 * NX)
            m1 = prod[:, :, :NX]
            t1 = sigma * pltpu.roll(prod[:, :, NX:], 4, 1)
            plus = (m1 + t1)[:GROUPS]
            minus = sigma * (m1 - t1)
            minus = jnp.where(first, minus[1 : GROUPS + 1], minus[:GROUPS])
            for b in range(BLOCKS):
                lanes = slice(b * LANES, (b + 1) * LANES)
                sbuf[pl.ds(GROUPS * chunk, GROUPS), b, p * 8 : p * 8 + 8, :] = plus[:, :, lanes]
                sbuf[pl.ds(64 + GROUPS * chunk, GROUPS), b, p * 8 : p * 8 + 8, :] = minus[:, :, lanes]

        @pl.when(i == 0)
        def _():
            pl.semaphore_wait(barrier, DEVICES - 1)

        def send(k, inner):
            half = k % 2
            a, e, o = (k // 2) % 4, (k // 8) % 2, k // 16
            within = 4 * ((y_at + a) % 4) + 2 * ((core + o) % 2) + (g + e) % 2
            to = jnp.where(half == 0, GROUPS * chunk + within, 64 + GROUPS * (3 - chunk) + within)
            slot = jnp.where(half == 0, GROUPS * chunk + within, 64 + GROUPS * chunk + 15 - within)

            @pl.when(to != me)
            def _():
                pltpu.make_async_remote_copy(
                    sbuf.at[slot], xbuf.at[g, :, pl.ds(16 * d, 16)], send_x, recv_x,
                    device_id=(to % 2, to // 2), device_id_type=MESH,
                ).start()

            @pl.when(to == me)
            def _():
                pltpu.make_async_copy(sbuf.at[slot], xbuf.at[g, :, pl.ds(16 * d, 16)], own_sem).start()

            return inner

        lax.fori_loop(0, 32, send, 0)
        return carry

    lax.fori_loop(0, CHUNKS, forward, 0)

    def row_of(j):
        return jnp.where(upper == 0, j, (4 - j) % 4)

    pltpu.make_async_copy(rin, rin, ref_sem).wait()
    for part in range(2):
        for j in range(ROWS):
            for b in range(BLOCKS):
                rbuf[part, b, :, j * LANES : (j + 1) * LANES] = rin[
                    b, part, pl.ds(4 * g + row_of(j), NZ, stride=8), :
                ]

    lane = lax.broadcasted_iota(jnp.int32, (8, WIDE), 1)
    j_of = lane // LANES
    ky = 8 * d + 4 * g + jnp.where(upper == 0, j_of, (4 - j_of) % 4)
    kz = lax.broadcasted_iota(jnp.int32, (NZ, LANES), 0)
    unit = 2.0 * math.pi / NX
    for which, source in enumerate((shifts, offsets)):
        for t in range(2):
            sign = -1.0 if which == 0 else 1.0
            phase = (kz * source[t, 0]) % NZ
            angle = (4.0 * unit) * phase.astype(F32)
            ramp_z[which, t, 0] = jnp.cos(angle)
            ramp_z[which, t, 1] = sign * jnp.sin(angle)
            for b in range(BLOCKS):
                kx = b * LANES + lane % LANES
                phase = (ky * source[t, 1] + kx * source[t, 2]) % NX
                angle = unit * phase.astype(F32)
                ramp_xy[which, t, b, 0] = jnp.cos(angle)
                ramp_xy[which, t, b, 1] = sign * jnp.sin(angle)

    def turned(which, t, b, re, im):
        zr, zs = ramp_z[which, t, 0], ramp_z[which, t, 1]
        xr = ramp_xy[which, t, b, 0][:1]
        xs = ramp_xy[which, t, b, 1][:1]
        out_re, out_im = [], []
        for j in range(ROWS):
            lanes = slice(j * LANES, (j + 1) * LANES)
            ar, ai = xr[:, lanes], xs[:, lanes]
            cr = zr * ar - zs * ai
            ci = zr * ai + zs * ar
            out_re.append(re[:, lanes] * cr - im[:, lanes] * ci)
            out_im.append(re[:, lanes] * ci + im[:, lanes] * cr)
        return jnp.concatenate(out_re, axis=1), jnp.concatenate(out_im, axis=1)

    pltpu.make_async_copy(sbuf.at[0], sbuf.at[0], own_sem).wait()
    pltpu.make_async_copy(sbuf.at[pl.ds(0, DEVICES - 1)], sbuf.at[pl.ds(0, DEVICES - 1)], recv_x).wait()

    def spectrum(b, sums):
        zh, zl = zf[0], zf[1]
        ref_re, ref_im = rbuf[0, b], rbuf[1, b]
        new_re, new_im = 0.5 * ref_re, 0.5 * ref_im
        found = []
        for t in range(2):
            re = [xbuf[t, b, pl.ds(j, NZ, stride=8), :] for j in range(ROWS)]
            im = [xbuf[t, b, pl.ds(4 + j, NZ, stride=8), :] for j in range(ROWS)]
            both = jnp.concatenate([jnp.concatenate(re, axis=1), jnp.concatenate(im, axis=1)], axis=0)
            bh, bl = split(both)
            freq = dot(zh, bh) + dot(zl, bh) + dot(zh, bl)
            fr, fi = freq[:NZ], freq[NZ:]
            cross_re = fr * ref_re + fi * ref_im
            cross_im = fi * ref_re - fr * ref_im
            magnitude = jnp.sqrt(cross_re * cross_re + cross_im * cross_im)
            cbuf[t, b, :NZ] = cross_re
            cbuf[t, b, NZ:] = cross_im
            mbuf[t, b] = magnitude
            found.append(sums[t] + magnitude.reshape(NZ // 8, 8, WIDE).sum(axis=0))
            wr, wi = turned(0, t, b, fr, fi)
            new_re += 0.25 * wr
            new_im += 0.25 * wi
        nbuf[b, 0] = new_re
        nbuf[b, 1] = new_im
        return tuple(found)

    sums = lax.fori_loop(0, BLOCKS, spectrum, (jnp.zeros((8, WIDE), F32),) * 2)

    lane1 = lax.broadcasted_iota(jnp.int32, (1, LANES), 1)
    mine[...] = jnp.where(lane1 < 64, jnp.sum(sums[0]), jnp.sum(sums[1]))

    def tell(k, carry):
        to = (me + k) % DEVICES
        pltpu.make_async_remote_copy(
            mine, abuf.at[me], send_a, recv_a, device_id=(to % 2, to // 2), device_id_type=MESH
        ).start()
        return carry

    lax.fori_loop(1, DEVICES, tell, 0)
    pltpu.make_async_copy(mine, abuf.at[me], own_sem).start()

    half = NZ // 2
    partner_copy = pltpu.make_async_remote_copy(
        nbuf.at[:, :, pl.ds((1 - g) * half, half)], nrecv, send_n, recv_n,
        device_id=(1 - g, d), device_id_type=MESH,
    )
    partner_copy.start()

    def keep(source, at_grp):
        for b in range(BLOCKS):
            for part in range(2):
                for j in range(ROWS):
                    nout[part, b, pl.ds(4 * at_grp + row_of(j), half, stride=8), :] = source[
                        b, part, :, j * LANES : (j + 1) * LANES
                    ]

    keep(nbuf.at[:, :, pl.ds(g * half, half)], g)

    pltpu.make_async_copy(mine, abuf.at[me], own_sem).wait()
    pltpu.make_async_copy(abuf.at[pl.ds(0, DEVICES - 1)], abuf.at[pl.ds(0, DEVICES - 1)], recv_a).wait()
    total = jnp.sum(abuf[...].reshape(DEVICES, LANES), axis=0, keepdims=True) / (NZ * NY * NX)

    def back(i, carry):
        t = (g + i) % 2
        average = jnp.sum(jnp.where(lane1 == 64 * t, total, 0.0))

        def whiten(b, inner):
            zh, zl = zi[0], zi[1]
            scale = 1.0 / (mbuf[t, b] + average)
            wr, wi = turned(1, t, b, cbuf[t, b, :NZ] * scale, cbuf[t, b, NZ:] * scale)
            both = jnp.concatenate([wr, wi], axis=0)
            bh, bl = split(both)
            depth = dot(zh, bh) + dot(zl, bh) + dot(zh, bl)
            dh, dl = split(depth)
            for part in range(2):
                for j in range(ROWS):
                    at = pl.ds(pl.multiple_of((2 * b + part) * LANES, LANES), LANES)
                    rows = slice(part * NZ, (part + 1) * NZ)
                    lanes = slice(j * LANES, (j + 1) * LANES)
                    g1hi[j * NZ : (j + 1) * NZ, at] = dh[rows, lanes]
                    g1lo[j * NZ : (j + 1) * NZ, at] = dl[rows, lanes]
            return inner

        lax.fori_loop(0, BLOCKS, whiten, 0)
        width = dot(g1hi[...], xi[0]) + dot(g1lo[...], xi[0]) + dot(g1hi[...], xi[1])
        for part in range(2):
            for j in range(ROWS):
                gbuf[t, pl.ds(4 * part + j, NZ, stride=8), :] = width[
                    j * NZ : (j + 1) * NZ, part * CROP : (part + 1) * CROP
                ]

        def send(k, inner):
            to = (d + k) % 64

            @pl.when((to != d) | (t != g))
            def _():
                pltpu.make_async_remote_copy(
                    gbuf.at[t, pl.ds(16 * to, 16)], ybuf.at[me], send_g, recv_g,
                    device_id=(t, to), device_id_type=MESH,
                ).start()

            @pl.when((to == d) & (t == g))
            def _():
                pltpu.make_async_copy(gbuf.at[t, pl.ds(16 * to, 16)], ybuf.at[me], own_sem).start()

            return inner

        lax.fori_loop(0, 64, send, 0)
        return carry

    lax.fori_loop(0, 2, back, 0)

    pltpu.make_async_copy(ybuf.at[0], ybuf.at[0], own_sem).wait()
    pltpu.make_async_copy(ybuf.at[pl.ds(0, DEVICES - 1)], ybuf.at[pl.ds(0, DEVICES - 1)], recv_g).wait()
    for p in range(2):
        rows = ybuf[:, p * 8 : p * 8 + 8, :].reshape(DEVICES * 8, CROP)
        rh, rl = split(rows)
        corr[p] = dot(yi[0], rh) + dot(yi[1], rh) + dot(yi[0], rl)

    partner_copy.wait_recv()
    keep(nrecv, 1 - g)

    pltpu.make_async_copy(sbuf.at[pl.ds(0, DEVICES - 1)], sbuf.at[pl.ds(0, DEVICES - 1)], send_x).wait()
    pltpu.make_async_copy(abuf.at[pl.ds(0, DEVICES - 1)], abuf.at[pl.ds(0, DEVICES - 1)], send_a).wait()
    pltpu.make_async_copy(ybuf.at[pl.ds(0, DEVICES - 1)], ybuf.at[pl.ds(0, DEVICES - 1)], send_g).wait()
    partner_copy.wait_send()


def local(frames, ref_spectrum, shifts, offsets):
    vmem = pl.BlockSpec(memory_space=pltpu.VMEM)
    smem = pl.BlockSpec(memory_space=pltpu.SMEM)
    corr, new = pl.pallas_call(
        kernel,
        out_shape=(
            jax.ShapeDtypeStruct((2, CROP, CROP), F32),
            jax.ShapeDtypeStruct((2, BLOCKS, NZ // 2 * 8, LANES), F32),
        ),
        in_specs=[vmem] * 7 + [smem] * 2 + [pl.BlockSpec(memory_space=pl.ANY)],
        out_specs=(vmem, vmem),
        scratch_shapes=[
            pltpu.VMEM((2, NY, NX), BF16),
            pltpu.VMEM((2, NY, NX), BF16),
            pltpu.VMEM((DEVICES, BLOCKS, 16, LANES), F32),
            pltpu.VMEM((2, BLOCKS, NZ * 8, LANES), F32),
            pltpu.VMEM((BLOCKS, 2, NZ * 8, LANES), F32),
            pltpu.VMEM((2, BLOCKS, NZ, WIDE), F32),
            pltpu.VMEM((2, BLOCKS, 2 * NZ, WIDE), F32),
            pltpu.VMEM((2, BLOCKS, NZ, WIDE), F32),
            pltpu.VMEM((BLOCKS, 2, NZ, WIDE), F32),
            pltpu.VMEM((BLOCKS, 2, NZ // 2, WIDE), F32),
            pltpu.VMEM((2, 2, BLOCKS, 2, 8, WIDE), F32),
            pltpu.VMEM((2, 2, 2, NZ, LANES), F32),
            pltpu.VMEM((1, LANES), F32),
            pltpu.VMEM((DEVICES, 1, LANES), F32),
            pltpu.VMEM((ROWS * NZ, 2 * NX), BF16),
            pltpu.VMEM((ROWS * NZ, 2 * NX), BF16),
            pltpu.VMEM((2, NZ * 8, LANES), F32),
            pltpu.VMEM((DEVICES, 16, LANES), F32),
        ]
        + [pltpu.SemaphoreType.DMA] * 10,
        compiler_params=pltpu.CompilerParams(
            collective_id=0, has_side_effects=True, vmem_limit_bytes=60 << 20
        ),
    )(
        frames[0],
        jnp.asarray(forward_y_table()),
        jnp.asarray(forward_x_table()),
        jnp.asarray(z_table(False)),
        jnp.asarray(z_table(True)),
        jnp.asarray(inverse_x_table()),
        jnp.asarray(inverse_y_table()),
        shifts,
        offsets,
        ref_spectrum.reshape(2, NZ * 8, NX),
    )
    new = new.reshape(2, BLOCKS, NZ // 2, 8, LANES).transpose(0, 2, 3, 1, 4)
    return corr[None], new.reshape(2, NZ // 2, 8, NX)


def solution(mesh):
    return jax.shard_map(
        local,
        mesh=mesh,
        in_specs=(P("grp", "dev", None, None), P(None, None, "dev", None), P(), P()),
        out_specs=(P("grp", "dev", None, None), P(None, "grp", "dev", None)),
        check_vma=False,
    )
```

```python
import math

import jax
import jax.numpy as jnp
import numpy as np
from jax import lax
from jax.experimental import pallas as pl
from jax.experimental.pallas import tpu as pltpu
from jax.sharding import PartitionSpec as P

NX = 512
NY = 512
NZ = 128
CROP = 128
ROWS = 4
LANES = 128
BLOCKS = NX // LANES
WIDE = ROWS * LANES
DEVICES = 128
CHUNKS = 4
GROUPS = 16
SPAN = (GROUPS + 4) * 8
FACTOR = 1.0 / math.sqrt(NZ * NY * NX)
F32 = jnp.float32
BF16 = jnp.bfloat16
MESH = pl.DeviceIdType.MESH


def halves(table):
    single = table.astype(np.float32)
    high = single.astype(jnp.bfloat16)
    low = (table - high.astype(np.float64)).astype(np.float32).astype(jnp.bfloat16)
    return np.stack([high, low])


def forward_y_table():
    out = np.zeros((CHUNKS, 4, 5, 2, ROWS, NY))
    y = np.arange(NY)
    for chunk in range(CHUNKS):
        for run in range(4):
            for at in range(5):
                for j in range(ROWS):
                    ky = 4 * (16 * run + 4 * ((chunk - run) % 4) + at) + j
                    angle = 2.0 * np.pi * (ky * y % NY) / NY
                    out[chunk, run, at, 0, j] = np.cos(angle)
                    out[chunk, run, at, 1, j] = -np.sin(angle)
    return halves(out.reshape(CHUNKS * SPAN, NY))


def forward_x_table():
    angle = 2.0 * np.pi * (np.arange(NX)[:, None] * np.arange(NX)[None, :] % NX) / NX
    return halves(np.concatenate([np.cos(angle), np.sin(angle)], axis=1))


def z_table(inverse):
    angle = 2.0 * np.pi * (np.arange(NZ)[:, None] * np.arange(NZ)[None, :] % NZ) / NZ
    c, s = np.cos(angle), np.sin(angle)
    if inverse:
        return halves(np.block([[c, -s], [s, c]]))
    return halves(FACTOR * np.block([[c, s], [-s, c]]))


def inverse_x_table():
    kx, x = np.arange(NX), np.arange(CROP)
    angle = 2.0 * np.pi * (kx[:, None] * x[None, :] % NX) / NX
    c, s = np.cos(angle), np.sin(angle)
    real = np.concatenate([c, s], axis=1).reshape(BLOCKS, LANES, 2 * CROP)
    imag = np.concatenate([-s, c], axis=1).reshape(BLOCKS, LANES, 2 * CROP)
    return halves(np.stack([real, imag], axis=1).reshape(2 * NX, 2 * CROP))


def inverse_y_table():
    group = np.arange(DEVICES)[:, None]
    j = np.arange(ROWS)[None, :]
    ky = 4 * group + np.where(group < DEVICES // 2, j, (4 - j) % 4)
    angle = 2.0 * np.pi * (np.arange(CROP)[:, None, None] * ky[None] % NY) / NY
    table = np.stack([np.cos(angle), -np.sin(angle)], axis=2)
    return halves(FACTOR * table.reshape(CROP, DEVICES * 8))


def split(a):
    high = a.astype(BF16)
    return high, (a - high.astype(F32)).astype(BF16)


def dot(a, b):
    return jnp.dot(a, b, preferred_element_type=F32)


def kernel(
    frames, dy, cs, zf, zi, xi, yi, shifts, offsets, ref_hbm,
    corr, nout,
    fhi, flo, sbuf, xbuf, rin, rbuf, cbuf, mbuf, nbuf, nrecv, ramp_xy, ramp_z,
    mine, abuf, g1hi, g1lo, gbuf, ybuf,
    send_x, recv_x, send_a, recv_a, send_n, recv_n, send_g, recv_g, ref_sem, own_sem,
):
    g = lax.axis_index("grp")
    d = lax.axis_index("dev")
    me = 2 * d + g
    core, y_at, z_at = d % 2, (d // 2) % 4, (d // 8) % 4
    upper = d // 32

    barrier = pltpu.get_barrier_semaphore()

    def greet(k, carry):
        to = (me + k) % DEVICES
        pl.semaphore_signal(barrier, 1, device_id=(to % 2, to // 2), device_id_type=MESH)
        return carry

    lax.fori_loop(1, DEVICES, greet, 0)
    for b in range(BLOCKS):
        pltpu.make_async_copy(ref_hbm.at[:, :, b * LANES : (b + 1) * LANES], rin.at[b], ref_sem).start()

    for p in range(2):
        high, low = split(frames[p])
        fhi[p] = high
        flo[p] = low

    sub = lax.broadcasted_iota(jnp.int32, (1, 8, NX), 1)
    sigma = jnp.where(sub < 4, 1.0, -1.0).astype(F32)
    first = (sub % 4) == 0

    def forward(i, carry):
        chunk = (y_at + z_at + i) % CHUNKS
        base = pl.multiple_of(chunk * SPAN, 16)
        dyh = dy[0, pl.ds(base, SPAN), :]
        dyl = dy[1, pl.ds(base, SPAN), :]
        for p in range(2):
            rows = dot(dyh, fhi[p]) + dot(dyh, flo[p]) + dot(dyl, fhi[p])
            rh, rl = split(rows)
            prod = dot(rh, cs[0]) + dot(rl, cs[0]) + dot(rh, cs[1])
            prod = prod.reshape(GROUPS + 4, 8, 2 * NX)
            m1 = prod[:, :, :NX]
            t1 = sigma * pltpu.roll(prod[:, :, NX:], 4, 1)
            plus = (m1 + t1).reshape(4, 5, 8, NX)[:, :4].reshape(GROUPS, 8, NX)
            minus = (sigma * (m1 - t1)).reshape(4, 5, 8, NX)
            minus = jnp.where(first[None], minus[:, 1:], minus[:, :4]).reshape(GROUPS, 8, NX)
            for b in range(BLOCKS):
                lanes = slice(b * LANES, (b + 1) * LANES)
                sbuf[pl.ds(GROUPS * chunk, GROUPS), b, p * 8 : p * 8 + 8, :] = plus[:, :, lanes]
                sbuf[pl.ds(64 + GROUPS * chunk, GROUPS), b, p * 8 : p * 8 + 8, :] = minus[:, :, lanes]

        @pl.when(i == 0)
        def _():
            pl.semaphore_wait(barrier, DEVICES - 1)

        def send(k, inner):
            half = (k + upper) % 2
            to_z = (z_at + k // 2) % 4
            to_y = jnp.where(half == 0, chunk + 8 - to_z, 10 - chunk - to_z) % 4
            within = 2 * ((core + k // 16) % 2) + (g + k // 8) % 2
            to = 64 * half + 16 * to_z + 4 * to_y + within
            slot = jnp.where(half == 0, GROUPS * chunk + 4 * to_z + within, 79 + GROUPS * chunk - 4 * to_z - within)

            @pl.when(to != me)
            def _():
                pltpu.make_async_remote_copy(
                    sbuf.at[slot], xbuf.at[g, :, pl.ds(16 * d, 16)], send_x, recv_x,
                    device_id=(to % 2, to // 2), device_id_type=MESH,
                ).start()

            @pl.when(to == me)
            def _():
                pltpu.make_async_copy(sbuf.at[slot], xbuf.at[g, :, pl.ds(16 * d, 16)], own_sem).start()

            return inner

        lax.fori_loop(0, 32, send, 0)
        return carry

    lax.fori_loop(0, CHUNKS, forward, 0)

    def row_of(j):
        return jnp.where(upper == 0, j, (4 - j) % 4)

    pltpu.make_async_copy(rin, rin, ref_sem).wait()
    for part in range(2):
        for j in range(ROWS):
            for b in range(BLOCKS):
                rbuf[part, b, :, j * LANES : (j + 1) * LANES] = rin[
                    b, part, pl.ds(4 * g + row_of(j), NZ, stride=8), :
                ]

    lane = lax.broadcasted_iota(jnp.int32, (8, WIDE), 1)
    j_of = lane // LANES
    ky = 8 * d + 4 * g + jnp.where(upper == 0, j_of, (4 - j_of) % 4)
    kz = lax.broadcasted_iota(jnp.int32, (NZ, LANES), 0)
    unit = 2.0 * math.pi / NX
    for which, source in enumerate((shifts, offsets)):
        for t in range(2):
            sign = -1.0 if which == 0 else 1.0
            phase = (kz * source[t, 0]) % NZ
            angle = (4.0 * unit) * phase.astype(F32)
            ramp_z[which, t, 0] = jnp.cos(angle)
            ramp_z[which, t, 1] = sign * jnp.sin(angle)
            for b in range(BLOCKS):
                kx = b * LANES + lane % LANES
                phase = (ky * source[t, 1] + kx * source[t, 2]) % NX
                angle = unit * phase.astype(F32)
                ramp_xy[which, t, b, 0] = jnp.cos(angle)
                ramp_xy[which, t, b, 1] = sign * jnp.sin(angle)

    def turned(which, t, b, re, im):
        zr, zs = ramp_z[which, t, 0], ramp_z[which, t, 1]
        xr = ramp_xy[which, t, b, 0][:1]
        xs = ramp_xy[which, t, b, 1][:1]
        out_re, out_im = [], []
        for j in range(ROWS):
            lanes = slice(j * LANES, (j + 1) * LANES)
            ar, ai = xr[:, lanes], xs[:, lanes]
            cr = zr * ar - zs * ai
            ci = zr * ai + zs * ar
            out_re.append(re[:, lanes] * cr - im[:, lanes] * ci)
            out_im.append(re[:, lanes] * ci + im[:, lanes] * cr)
        return jnp.concatenate(out_re, axis=1), jnp.concatenate(out_im, axis=1)

    pltpu.make_async_copy(sbuf.at[0], sbuf.at[0], own_sem).wait()
    pltpu.make_async_copy(sbuf.at[pl.ds(0, DEVICES - 1)], sbuf.at[pl.ds(0, DEVICES - 1)], recv_x).wait()

    half = NZ // 2

    def to_partner(b):
        return pltpu.make_async_remote_copy(
            nbuf.at[b, :, pl.ds((1 - g) * half, half)], nrecv.at[b], send_n, recv_n,
            device_id=(1 - g, d), device_id_type=MESH,
        )

    def spectrum(b, sums):
        zh, zl = zf[0], zf[1]
        ref_re, ref_im = rbuf[0, b], rbuf[1, b]
        new_re, new_im = 0.5 * ref_re, 0.5 * ref_im
        found = []
        for t in range(2):
            re = [xbuf[t, b, pl.ds(j, NZ, stride=8), :] for j in range(ROWS)]
            im = [xbuf[t, b, pl.ds(4 + j, NZ, stride=8), :] for j in range(ROWS)]
            both = jnp.concatenate([jnp.concatenate(re, axis=1), jnp.concatenate(im, axis=1)], axis=0)
            bh, bl = split(both)
            freq = dot(zh, bh) + dot(zl, bh) + dot(zh, bl)
            fr, fi = freq[:NZ], freq[NZ:]
            cross_re = fr * ref_re + fi * ref_im
            cross_im = fi * ref_re - fr * ref_im
            magnitude = jnp.sqrt(cross_re * cross_re + cross_im * cross_im)
            cbuf[t, b, :NZ] = cross_re
            cbuf[t, b, NZ:] = cross_im
            mbuf[t, b] = magnitude
            found.append(sums[t] + magnitude.reshape(NZ // 8, 8, WIDE).sum(axis=0))
            wr, wi = turned(0, t, b, fr, fi)
            new_re += 0.25 * wr
            new_im += 0.25 * wi
        nbuf[b, 0] = new_re
        nbuf[b, 1] = new_im

        @pl.when(b == 0)
        def _():
            to_partner(b).start()

        return tuple(found)

    sums = lax.fori_loop(0, BLOCKS, spectrum, (jnp.zeros((8, WIDE), F32),) * 2)

    lane1 = lax.broadcasted_iota(jnp.int32, (1, LANES), 1)
    mine[...] = jnp.where(lane1 < 64, jnp.sum(sums[0]), jnp.sum(sums[1]))

    def tell(k, carry):
        to = (me + k) % DEVICES
        pltpu.make_async_remote_copy(
            mine, abuf.at[me], send_a, recv_a, device_id=(to % 2, to // 2), device_id_type=MESH
        ).start()
        return carry

    lax.fori_loop(1, DEVICES, tell, 0)
    pltpu.make_async_copy(mine, abuf.at[me], own_sem).start()

    for b in range(1, BLOCKS):
        to_partner(b).start()

    def keep(source, at_grp):
        for b in range(BLOCKS):
            for part in range(2):
                for j in range(ROWS):
                    nout[part, b, pl.ds(4 * at_grp + row_of(j), half, stride=8), :] = source[
                        b, part, :, j * LANES : (j + 1) * LANES
                    ]

    keep(nbuf.at[:, :, pl.ds(g * half, half)], g)

    pltpu.make_async_copy(mine, abuf.at[me], own_sem).wait()
    pltpu.make_async_copy(abuf.at[pl.ds(0, DEVICES - 1)], abuf.at[pl.ds(0, DEVICES - 1)], recv_a).wait()
    total = jnp.sum(abuf[...].reshape(DEVICES, LANES), axis=0, keepdims=True) / (NZ * NY * NX)

    def back(i, carry):
        t = (g + i) % 2
        average = jnp.sum(jnp.where(lane1 == 64 * t, total, 0.0))

        def whiten(b, inner):
            zh, zl = zi[0], zi[1]
            scale = 1.0 / (mbuf[t, b] + average)
            wr, wi = turned(1, t, b, cbuf[t, b, :NZ] * scale, cbuf[t, b, NZ:] * scale)
            both = jnp.concatenate([wr, wi], axis=0)
            bh, bl = split(both)
            depth = dot(zh, bh) + dot(zl, bh) + dot(zh, bl)
            dh, dl = split(depth)
            for part in range(2):
                for j in range(ROWS):
                    at = pl.ds(pl.multiple_of((2 * b + part) * LANES, LANES), LANES)
                    rows = slice(part * NZ, (part + 1) * NZ)
                    lanes = slice(j * LANES, (j + 1) * LANES)
                    g1hi[j * NZ : (j + 1) * NZ, at] = dh[rows, lanes]
                    g1lo[j * NZ : (j + 1) * NZ, at] = dl[rows, lanes]
            return inner

        lax.fori_loop(0, BLOCKS, whiten, 0)
        width = dot(g1hi[...], xi[0]) + dot(g1lo[...], xi[0]) + dot(g1hi[...], xi[1])
        for part in range(2):
            for j in range(ROWS):
                gbuf[t, pl.ds(4 * part + j, NZ, stride=8), :] = width[
                    j * NZ : (j + 1) * NZ, part * CROP : (part + 1) * CROP
                ]

        def send(k, inner):
            to = (d + k) % 64

            @pl.when((to != d) | (t != g))
            def _():
                pltpu.make_async_remote_copy(
                    gbuf.at[t, pl.ds(16 * to, 16)], ybuf.at[me], send_g, recv_g,
                    device_id=(t, to), device_id_type=MESH,
                ).start()

            @pl.when((to == d) & (t == g))
            def _():
                pltpu.make_async_copy(gbuf.at[t, pl.ds(16 * to, 16)], ybuf.at[me], own_sem).start()

            return inner

        lax.fori_loop(0, 64, send, 0)
        return carry

    lax.fori_loop(0, 2, back, 0)

    pltpu.make_async_copy(ybuf.at[0], ybuf.at[0], own_sem).wait()
    pltpu.make_async_copy(ybuf.at[pl.ds(0, DEVICES - 1)], ybuf.at[pl.ds(0, DEVICES - 1)], recv_g).wait()
    for p in range(2):
        rows = ybuf[:, p * 8 : p * 8 + 8, :].reshape(DEVICES * 8, CROP)
        rh, rl = split(rows)
        corr[p] = dot(yi[0], rh) + dot(yi[1], rh) + dot(yi[0], rl)

    pltpu.make_async_copy(nrecv, nrecv, recv_n).wait()
    keep(nrecv, 1 - g)

    pltpu.make_async_copy(sbuf.at[pl.ds(0, DEVICES - 1)], sbuf.at[pl.ds(0, DEVICES - 1)], send_x).wait()
    pltpu.make_async_copy(abuf.at[pl.ds(0, DEVICES - 1)], abuf.at[pl.ds(0, DEVICES - 1)], send_a).wait()
    pltpu.make_async_copy(ybuf.at[pl.ds(0, DEVICES - 1)], ybuf.at[pl.ds(0, DEVICES - 1)], send_g).wait()
    pltpu.make_async_copy(nrecv, nrecv, send_n).wait()


def local(frames, ref_spectrum, shifts, offsets):
    vmem = pl.BlockSpec(memory_space=pltpu.VMEM)
    smem = pl.BlockSpec(memory_space=pltpu.SMEM)
    corr, new = pl.pallas_call(
        kernel,
        out_shape=(
            jax.ShapeDtypeStruct((2, CROP, CROP), F32),
            jax.ShapeDtypeStruct((2, BLOCKS, NZ // 2 * 8, LANES), F32),
        ),
        in_specs=[vmem] * 7 + [smem] * 2 + [pl.BlockSpec(memory_space=pl.ANY)],
        out_specs=(vmem, vmem),
        scratch_shapes=[
            pltpu.VMEM((2, NY, NX), BF16),
            pltpu.VMEM((2, NY, NX), BF16),
            pltpu.VMEM((DEVICES, BLOCKS, 16, LANES), F32),
            pltpu.VMEM((2, BLOCKS, NZ * 8, LANES), F32),
            pltpu.VMEM((BLOCKS, 2, NZ * 8, LANES), F32),
            pltpu.VMEM((2, BLOCKS, NZ, WIDE), F32),
            pltpu.VMEM((2, BLOCKS, 2 * NZ, WIDE), F32),
            pltpu.VMEM((2, BLOCKS, NZ, WIDE), F32),
            pltpu.VMEM((BLOCKS, 2, NZ, WIDE), F32),
            pltpu.VMEM((BLOCKS, 2, NZ // 2, WIDE), F32),
            pltpu.VMEM((2, 2, BLOCKS, 2, 8, WIDE), F32),
            pltpu.VMEM((2, 2, 2, NZ, LANES), F32),
            pltpu.VMEM((1, LANES), F32),
            pltpu.VMEM((DEVICES, 1, LANES), F32),
            pltpu.VMEM((ROWS * NZ, 2 * NX), BF16),
            pltpu.VMEM((ROWS * NZ, 2 * NX), BF16),
            pltpu.VMEM((2, NZ * 8, LANES), F32),
            pltpu.VMEM((DEVICES, 16, LANES), F32),
        ]
        + [pltpu.SemaphoreType.DMA] * 10,
        compiler_params=pltpu.CompilerParams(
            collective_id=0, has_side_effects=True, vmem_limit_bytes=60 << 20
        ),
    )(
        frames[0],
        jnp.asarray(forward_y_table()),
        jnp.asarray(forward_x_table()),
        jnp.asarray(z_table(False)),
        jnp.asarray(z_table(True)),
        jnp.asarray(inverse_x_table()),
        jnp.asarray(inverse_y_table()),
        shifts,
        offsets,
        ref_spectrum.reshape(2, NZ * 8, NX),
    )
    new = new.reshape(2, BLOCKS, NZ // 2, 8, LANES).transpose(0, 2, 3, 1, 4)
    return corr[None], new.reshape(2, NZ // 2, 8, NX)


def solution(mesh):
    return jax.shard_map(
        local,
        mesh=mesh,
        in_specs=(P("grp", "dev", None, None), P(None, None, "dev", None), P(), P()),
        out_specs=(P("grp", "dev", None, None), P(None, "grp", "dev", None)),
        check_vma=False,
    )
```

```python
import math

import jax
import jax.numpy as jnp
import numpy as np
from jax import lax
from jax.experimental import pallas as pl
from jax.experimental.pallas import tpu as pltpu
from jax.sharding import PartitionSpec as P

NX = 512
NY = 512
NZ = 128
CROP = 128
ROWS = 4
LANES = 128
BLOCKS = NX // LANES
WIDE = ROWS * LANES
DEVICES = 128
CHUNKS = 4
GROUPS = 16
SPAN = (GROUPS + 4) * 8
FACTOR = 1.0 / math.sqrt(NZ * NY * NX)
F32 = jnp.float32
BF16 = jnp.bfloat16
MESH = pl.DeviceIdType.MESH


def halves(table):
    single = table.astype(np.float32)
    high = single.astype(jnp.bfloat16)
    low = (table - high.astype(np.float64)).astype(np.float32).astype(jnp.bfloat16)
    return np.stack([high, low])


def forward_y_table():
    out = np.zeros((CHUNKS, 4, 5, 2, ROWS, NY))
    y = np.arange(NY)
    for chunk in range(CHUNKS):
        for run in range(4):
            for at in range(5):
                for j in range(ROWS):
                    ky = 4 * (16 * run + 4 * ((chunk - run) % 4) + at) + j
                    angle = 2.0 * np.pi * (ky * y % NY) / NY
                    out[chunk, run, at, 0, j] = np.cos(angle)
                    out[chunk, run, at, 1, j] = -np.sin(angle)
    return halves(out.reshape(CHUNKS * SPAN, NY))


def forward_x_table():
    angle = 2.0 * np.pi * (np.arange(NX)[:, None] * np.arange(NX)[None, :] % NX) / NX
    return halves(np.concatenate([np.cos(angle), np.sin(angle)], axis=1))


def z_table(inverse):
    angle = 2.0 * np.pi * (np.arange(NZ)[:, None] * np.arange(NZ)[None, :] % NZ) / NZ
    c, s = np.cos(angle), np.sin(angle)
    if inverse:
        return halves(np.block([[c, -s], [s, c]]))
    return halves(FACTOR * np.block([[c, s], [-s, c]]))


def inverse_x_table():
    kx, x = np.arange(NX), np.arange(CROP)
    angle = 2.0 * np.pi * (kx[:, None] * x[None, :] % NX) / NX
    c, s = np.cos(angle), np.sin(angle)
    real = np.concatenate([c, s], axis=1).reshape(BLOCKS, LANES, 2 * CROP)
    imag = np.concatenate([-s, c], axis=1).reshape(BLOCKS, LANES, 2 * CROP)
    return halves(np.stack([real, imag], axis=1).reshape(2 * NX, 2 * CROP))


def inverse_y_table():
    group = np.arange(DEVICES)[:, None]
    j = np.arange(ROWS)[None, :]
    ky = 4 * group + np.where(group < DEVICES // 2, j, (4 - j) % 4)
    angle = 2.0 * np.pi * (np.arange(CROP)[:, None, None] * ky[None] % NY) / NY
    table = np.stack([np.cos(angle), -np.sin(angle)], axis=2)
    return halves(FACTOR * table.reshape(CROP, DEVICES * 8))


def split(a):
    high = a.astype(BF16)
    return high, (a - high.astype(F32)).astype(BF16)


def dot(a, b):
    return jnp.dot(a, b, preferred_element_type=F32)


def kernel(
    frames_hbm, dy_hbm, cs_hbm, zf_hbm, zi_hbm, xi_hbm, yi_hbm, shifts_hbm, offsets_hbm, ref_hbm,
    corr, nout,
    frames, dy, cs, zf, zi, xi, yi, shifts, offsets,
    fhi, flo, sbuf, xbuf, rin, rbuf, cbuf, mbuf, nbuf, nrecv, ramp_xy, ramp_z,
    mine, abuf, g1hi, g1lo, gbuf, ybuf,
    send_x, recv_x, send_a, recv_a, send_n, recv_n, send_g, recv_g, ref_sem, own_sem,
    recv_y, first_sem, table_sem,
):
    g = lax.axis_index("grp")
    d = lax.axis_index("dev")
    me = 2 * d + g
    core, y_at, z_at = d % 2, (d // 2) % 4, (d // 8) % 4
    upper = d // 32

    barrier = pltpu.get_barrier_semaphore()

    early = [(frames_hbm, frames), (dy_hbm, dy), (cs_hbm, cs)]
    late = [(zf_hbm, zf), (zi_hbm, zi), (xi_hbm, xi), (yi_hbm, yi), (shifts_hbm, shifts), (offsets_hbm, offsets)]
    early = [pltpu.make_async_copy(a, b, first_sem.at[i]) for i, (a, b) in enumerate(early)]
    late = [pltpu.make_async_copy(a, b, table_sem.at[i]) for i, (a, b) in enumerate(late)]
    for copy in early:
        copy.start()

    def greet(k, carry):
        to = (me + 104 + k + jnp.where(k >= 24, 1, 0)) % DEVICES
        pl.semaphore_signal(barrier, 1, device_id=(to % 2, to // 2), device_id_type=MESH)
        return carry

    lax.fori_loop(0, DEVICES - 1, greet, 0)
    for copy in late:
        copy.start()
    for b in range(BLOCKS):
        pltpu.make_async_copy(ref_hbm.at[:, :, b * LANES : (b + 1) * LANES], rin.at[b], ref_sem).start()

    early[0].wait()
    for p in range(2):
        high, low = split(frames[p])
        fhi[p] = high
        flo[p] = low

    early[1].wait()
    early[2].wait()
    sub = lax.broadcasted_iota(jnp.int32, (1, 8, NX), 1)
    sigma = jnp.where(sub < 4, 1.0, -1.0).astype(F32)
    first = (sub % 4) == 0

    pair = BLOCKS // 2

    def send(chunk, k, which):
        half = (k + upper) % 2
        to_z = (z_at + k // 2) % 4
        to_y = jnp.where(half == 0, chunk + 8 - to_z, 10 - chunk - to_z) % 4
        within = 2 * ((core + k // 16) % 2) + (g + k // 8) % 2
        to = 64 * half + 16 * to_z + 4 * to_y + within
        slot = jnp.where(half == 0, GROUPS * chunk + 4 * to_z + within, 79 + GROUPS * chunk - 4 * to_z - within)
        blocks = slice(which * pair, (which + 1) * pair)
        source, target = sbuf.at[slot, blocks], xbuf.at[g, blocks, pl.ds(16 * d, 16)]

        @pl.when(to != me)
        def _():
            pltpu.make_async_remote_copy(
                source, target, send_x, recv_y if which else recv_x,
                device_id=(to % 2, to // 2), device_id_type=MESH,
            ).start()

        @pl.when(to == me)
        def _():
            pltpu.make_async_copy(source, target, own_sem).start()

        return 0

    def forward(i, carry):
        chunk = (y_at + z_at + i) % CHUNKS
        base = pl.multiple_of(chunk * SPAN, 16)
        dyh = dy[0, pl.ds(base, SPAN), :]
        dyl = dy[1, pl.ds(base, SPAN), :]
        for p in range(2):
            rows = dot(dyh, fhi[p]) + dot(dyh, flo[p]) + dot(dyl, fhi[p])
            rh, rl = split(rows)
            prod = dot(rh, cs[0]) + dot(rl, cs[0]) + dot(rh, cs[1])
            prod = prod.reshape(GROUPS + 4, 8, 2 * NX)
            m1 = prod[:, :, :NX]
            t1 = sigma * pltpu.roll(prod[:, :, NX:], 4, 1)
            plus = (m1 + t1).reshape(4, 5, 8, NX)[:, :4].reshape(GROUPS, 8, NX)
            minus = (sigma * (m1 - t1)).reshape(4, 5, 8, NX)
            minus = jnp.where(first[None], minus[:, 1:], minus[:, :4]).reshape(GROUPS, 8, NX)
            for b in range(BLOCKS):
                lanes = slice(b * LANES, (b + 1) * LANES)
                sbuf[pl.ds(GROUPS * chunk, GROUPS), b, p * 8 : p * 8 + 8, :] = plus[:, :, lanes]
                sbuf[pl.ds(64 + GROUPS * chunk, GROUPS), b, p * 8 : p * 8 + 8, :] = minus[:, :, lanes]

        @pl.when(i == 0)
        def _():
            pl.semaphore_wait(barrier, DEVICES - 1)

        lax.fori_loop(0, 32, lambda k, inner: send(chunk, k, 0), 0)
        return carry

    lax.fori_loop(0, CHUNKS, forward, 0)
    lax.fori_loop(0, 32 * CHUNKS, lambda k, inner: send((y_at + z_at + k // 32) % CHUNKS, k % 32, 1), 0)

    def row_of(j):
        return jnp.where(upper == 0, j, (4 - j) % 4)

    for copy in late:
        copy.wait()
    pltpu.make_async_copy(rin, rin, ref_sem).wait()
    for part in range(2):
        for j in range(ROWS):
            for b in range(BLOCKS):
                rbuf[part, b, :, j * LANES : (j + 1) * LANES] = rin[
                    b, part, pl.ds(4 * g + row_of(j), NZ, stride=8), :
                ]

    lane = lax.broadcasted_iota(jnp.int32, (8, WIDE), 1)
    j_of = lane // LANES
    ky = 8 * d + 4 * g + jnp.where(upper == 0, j_of, (4 - j_of) % 4)
    kz = lax.broadcasted_iota(jnp.int32, (NZ, LANES), 0)
    unit = 2.0 * math.pi / NX
    for which, source in enumerate((shifts, offsets)):
        for t in range(2):
            sign = -1.0 if which == 0 else 1.0
            phase = (kz * source[t, 0]) % NZ
            angle = (4.0 * unit) * phase.astype(F32)
            ramp_z[which, t, 0] = jnp.cos(angle)
            ramp_z[which, t, 1] = sign * jnp.sin(angle)
            for b in range(BLOCKS):
                kx = b * LANES + lane % LANES
                phase = (ky * source[t, 1] + kx * source[t, 2]) % NX
                angle = unit * phase.astype(F32)
                ramp_xy[which, t, b, 0] = jnp.cos(angle)
                ramp_xy[which, t, b, 1] = sign * jnp.sin(angle)

    def turned(which, t, b, re, im):
        zr, zs = ramp_z[which, t, 0], ramp_z[which, t, 1]
        xr = ramp_xy[which, t, b, 0][:1]
        xs = ramp_xy[which, t, b, 1][:1]
        out_re, out_im = [], []
        for j in range(ROWS):
            lanes = slice(j * LANES, (j + 1) * LANES)
            ar, ai = xr[:, lanes], xs[:, lanes]
            cr = zr * ar - zs * ai
            ci = zr * ai + zs * ar
            out_re.append(re[:, lanes] * cr - im[:, lanes] * ci)
            out_im.append(re[:, lanes] * ci + im[:, lanes] * cr)
        return jnp.concatenate(out_re, axis=1), jnp.concatenate(out_im, axis=1)

    pltpu.make_async_copy(sbuf.at[0], sbuf.at[0], own_sem).wait()
    arrivals = sbuf.at[pl.ds(0, DEVICES - 1), 0:pair]
    pltpu.make_async_copy(arrivals, arrivals, recv_x).wait()

    half = NZ // 2

    def to_partner(b):
        return pltpu.make_async_remote_copy(
            nbuf.at[b, :, pl.ds((1 - g) * half, half)], nrecv.at[b], send_n, recv_n,
            device_id=(1 - g, d), device_id_type=MESH,
        )

    def spectrum(b, sums):
        @pl.when(b == pair)
        def _():
            pltpu.make_async_copy(arrivals, arrivals, recv_y).wait()

        zh, zl = zf[0], zf[1]
        ref_re, ref_im = rbuf[0, b], rbuf[1, b]
        new_re, new_im = 0.5 * ref_re, 0.5 * ref_im
        found = []
        for t in range(2):
            re = [xbuf[t, b, pl.ds(j, NZ, stride=8), :] for j in range(ROWS)]
            im = [xbuf[t, b, pl.ds(4 + j, NZ, stride=8), :] for j in range(ROWS)]
            both = jnp.concatenate([jnp.concatenate(re, axis=1), jnp.concatenate(im, axis=1)], axis=0)
            bh, bl = split(both)
            freq = dot(zh, bh) + dot(zl, bh) + dot(zh, bl)
            fr, fi = freq[:NZ], freq[NZ:]
            cross_re = fr * ref_re + fi * ref_im
            cross_im = fi * ref_re - fr * ref_im
            magnitude = jnp.sqrt(cross_re * cross_re + cross_im * cross_im)
            cbuf[t, b, :NZ] = cross_re
            cbuf[t, b, NZ:] = cross_im
            mbuf[t, b] = magnitude
            found.append(sums[t] + magnitude.reshape(NZ // 8, 8, WIDE).sum(axis=0))
            wr, wi = turned(0, t, b, fr, fi)
            new_re += 0.25 * wr
            new_im += 0.25 * wi
        nbuf[b, 0] = new_re
        nbuf[b, 1] = new_im

        @pl.when(b == 0)
        def _():
            to_partner(b).start()

        return tuple(found)

    sums = lax.fori_loop(0, BLOCKS, spectrum, (jnp.zeros((8, WIDE), F32),) * 2)

    lane1 = lax.broadcasted_iota(jnp.int32, (1, LANES), 1)
    mine[...] = jnp.where(lane1 < 64, jnp.sum(sums[0]), jnp.sum(sums[1]))

    def tell(k, carry):
        to = (me + k) % DEVICES
        pltpu.make_async_remote_copy(
            mine, abuf.at[me], send_a, recv_a, device_id=(to % 2, to // 2), device_id_type=MESH
        ).start()
        return carry

    lax.fori_loop(1, DEVICES, tell, 0)
    pltpu.make_async_copy(mine, abuf.at[me], own_sem).start()

    for b in range(1, BLOCKS):
        to_partner(b).start()

    def keep(source, at_grp):
        for b in range(BLOCKS):
            for part in range(2):
                for j in range(ROWS):
                    nout[part, pl.ds(8 * b + 4 * at_grp + row_of(j), half, stride=8 * BLOCKS), :] = source[
                        b, part, :, j * LANES : (j + 1) * LANES
                    ]

    keep(nbuf.at[:, :, pl.ds(g * half, half)], g)

    pltpu.make_async_copy(mine, abuf.at[me], own_sem).wait()
    pltpu.make_async_copy(abuf.at[pl.ds(0, DEVICES - 1)], abuf.at[pl.ds(0, DEVICES - 1)], recv_a).wait()
    total = jnp.sum(abuf[...].reshape(DEVICES, LANES), axis=0, keepdims=True) / (NZ * NY * NX)

    def back(i, carry):
        t = (g + i) % 2
        average = jnp.sum(jnp.where(lane1 == 64 * t, total, 0.0))

        def whiten(b, inner):
            zh, zl = zi[0], zi[1]
            scale = 1.0 / (mbuf[t, b] + average)
            wr, wi = turned(1, t, b, cbuf[t, b, :NZ] * scale, cbuf[t, b, NZ:] * scale)
            both = jnp.concatenate([wr, wi], axis=0)
            bh, bl = split(both)
            depth = dot(zh, bh) + dot(zl, bh) + dot(zh, bl)
            dh, dl = split(depth)
            for part in range(2):
                for j in range(ROWS):
                    at = pl.ds(pl.multiple_of((2 * b + part) * LANES, LANES), LANES)
                    rows = slice(part * NZ, (part + 1) * NZ)
                    lanes = slice(j * LANES, (j + 1) * LANES)
                    g1hi[j * NZ : (j + 1) * NZ, at] = dh[rows, lanes]
                    g1lo[j * NZ : (j + 1) * NZ, at] = dl[rows, lanes]
            return inner

        lax.fori_loop(0, BLOCKS, whiten, 0)
        width = dot(g1hi[...], xi[0]) + dot(g1lo[...], xi[0]) + dot(g1hi[...], xi[1])
        for part in range(2):
            for j in range(ROWS):
                gbuf[t, pl.ds(4 * part + j, NZ, stride=8), :] = width[
                    j * NZ : (j + 1) * NZ, part * CROP : (part + 1) * CROP
                ]

        def send(k, inner):
            to = (d + k) % 64

            @pl.when((to != d) | (t != g))
            def _():
                pltpu.make_async_remote_copy(
                    gbuf.at[t, pl.ds(16 * to, 16)], ybuf.at[me], send_g, recv_g,
                    device_id=(t, to), device_id_type=MESH,
                ).start()

            @pl.when((to == d) & (t == g))
            def _():
                pltpu.make_async_copy(gbuf.at[t, pl.ds(16 * to, 16)], ybuf.at[me], own_sem).start()

            return inner

        lax.fori_loop(0, 64, send, 0)
        return carry

    lax.fori_loop(0, 2, back, 0)

    pltpu.make_async_copy(ybuf.at[0], ybuf.at[0], own_sem).wait()
    pltpu.make_async_copy(ybuf.at[pl.ds(0, DEVICES - 1)], ybuf.at[pl.ds(0, DEVICES - 1)], recv_g).wait()
    for p in range(2):
        rows = ybuf[:, p * 8 : p * 8 + 8, :].reshape(DEVICES * 8, CROP)
        rh, rl = split(rows)
        corr[p] = dot(yi[0], rh) + dot(yi[1], rh) + dot(yi[0], rl)

    pltpu.make_async_copy(nrecv, nrecv, recv_n).wait()
    keep(nrecv, 1 - g)

    pltpu.make_async_copy(sbuf.at[pl.ds(0, DEVICES - 1)], sbuf.at[pl.ds(0, DEVICES - 1)], send_x).wait()
    pltpu.make_async_copy(abuf.at[pl.ds(0, DEVICES - 1)], abuf.at[pl.ds(0, DEVICES - 1)], send_a).wait()
    pltpu.make_async_copy(ybuf.at[pl.ds(0, DEVICES - 1)], ybuf.at[pl.ds(0, DEVICES - 1)], send_g).wait()
    pltpu.make_async_copy(nrecv, nrecv, send_n).wait()


def local(frames, ref_spectrum, shifts, offsets):
    vmem = pl.BlockSpec(memory_space=pltpu.VMEM)
    hbm = pl.BlockSpec(memory_space=pltpu.HBM)
    corr, new = pl.pallas_call(
        kernel,
        out_shape=(
            jax.ShapeDtypeStruct((2, CROP, CROP), F32),
            jax.ShapeDtypeStruct((2, NZ // 2 * BLOCKS * 8, LANES), F32),
        ),
        in_specs=[hbm] * 10,
        out_specs=(vmem, vmem),
        scratch_shapes=[
            pltpu.VMEM((2, NY, NX), F32),
            pltpu.VMEM((2, CHUNKS * SPAN, NY), BF16),
            pltpu.VMEM((2, NX, 2 * NX), BF16),
            pltpu.VMEM((2, 2 * NZ, 2 * NZ), BF16),
            pltpu.VMEM((2, 2 * NZ, 2 * NZ), BF16),
            pltpu.VMEM((2, 2 * NX, 2 * CROP), BF16),
            pltpu.VMEM((2, CROP, DEVICES * 8), BF16),
            pltpu.SMEM((2, 3), jnp.int32),
            pltpu.SMEM((2, 3), jnp.int32),
            pltpu.VMEM((2, NY, NX), BF16),
            pltpu.VMEM((2, NY, NX), BF16),
            pltpu.VMEM((DEVICES, BLOCKS, 16, LANES), F32),
            pltpu.VMEM((2, BLOCKS, NZ * 8, LANES), F32),
            pltpu.VMEM((BLOCKS, 2, NZ * 8, LANES), F32),
            pltpu.VMEM((2, BLOCKS, NZ, WIDE), F32),
            pltpu.VMEM((2, BLOCKS, 2 * NZ, WIDE), F32),
            pltpu.VMEM((2, BLOCKS, NZ, WIDE), F32),
            pltpu.VMEM((BLOCKS, 2, NZ, WIDE), F32),
            pltpu.VMEM((BLOCKS, 2, NZ // 2, WIDE), F32),
            pltpu.VMEM((2, 2, BLOCKS, 2, 8, WIDE), F32),
            pltpu.VMEM((2, 2, 2, NZ, LANES), F32),
            pltpu.VMEM((1, LANES), F32),
            pltpu.VMEM((DEVICES, 1, LANES), F32),
            pltpu.VMEM((ROWS * NZ, 2 * NX), BF16),
            pltpu.VMEM((ROWS * NZ, 2 * NX), BF16),
            pltpu.VMEM((2, NZ * 8, LANES), F32),
            pltpu.VMEM((DEVICES, 16, LANES), F32),
        ]
        + [pltpu.SemaphoreType.DMA] * 11
        + [pltpu.SemaphoreType.DMA((3,)), pltpu.SemaphoreType.DMA((6,))],
        compiler_params=pltpu.CompilerParams(
            collective_id=0, has_side_effects=True, vmem_limit_bytes=46 << 20
        ),
    )(
        *(
            pltpu.with_memory_space_constraint(x, pltpu.HBM)
            for x in (
                frames[0],
                jnp.asarray(forward_y_table()),
                jnp.asarray(forward_x_table()),
                jnp.asarray(z_table(False)),
                jnp.asarray(z_table(True)),
                jnp.asarray(inverse_x_table()),
                jnp.asarray(inverse_y_table()),
                shifts,
                offsets,
                ref_spectrum.reshape(2, NZ * 8, NX),
            )
        )
    )
    new = new.reshape(2, NZ // 2, BLOCKS, 8, LANES).transpose(0, 1, 3, 2, 4)
    return corr[None], new.reshape(2, NZ // 2, 8, NX)


def solution(mesh):
    return jax.shard_map(
        local,
        mesh=mesh,
        in_specs=(P("grp", "dev", None, None), P(None, None, "dev", None), P(), P()),
        out_specs=(P("grp", "dev", None, None), P(None, "grp", "dev", None)),
        check_vma=False,
    )
```

```python
import math

import jax
import jax.numpy as jnp
import numpy as np
from jax import lax
from jax.experimental import pallas as pl
from jax.experimental.pallas import tpu as pltpu
from jax.sharding import PartitionSpec as P

NX = 512
NY = 512
NZ = 128
CROP = 128
ROWS = 4
LANES = 128
BLOCKS = NX // LANES
WIDE = ROWS * LANES
DEVICES = 128
CHUNKS = 4
GROUPS = 16
SPAN = (GROUPS + 4) * 8
FACTOR = 1.0 / math.sqrt(NZ * NY * NX)
F32 = jnp.float32
BF16 = jnp.bfloat16
MESH = pl.DeviceIdType.MESH
UNROLL = 8
EARLY = 2
PASS = 2


def halves(table):
    single = table.astype(np.float32)
    high = single.astype(jnp.bfloat16)
    low = (table - high.astype(np.float64)).astype(np.float32).astype(jnp.bfloat16)
    return np.stack([high, low])


def forward_y_table():
    out = np.zeros((CHUNKS, 4, 5, 2, ROWS, NY))
    y = np.arange(NY)
    for chunk in range(CHUNKS):
        for run in range(4):
            for at in range(5):
                for j in range(ROWS):
                    ky = 4 * (16 * run + 4 * ((chunk - run) % 4) + at) + j
                    angle = 2.0 * np.pi * (ky * y % NY) / NY
                    out[chunk, run, at, 0, j] = np.cos(angle)
                    out[chunk, run, at, 1, j] = -np.sin(angle)
    return halves(out.reshape(CHUNKS * SPAN, NY))


def forward_x_table():
    angle = 2.0 * np.pi * (np.arange(NX)[:, None] * np.arange(NX)[None, :] % NX) / NX
    return halves(np.concatenate([np.cos(angle), np.sin(angle)], axis=1))


def z_table(inverse):
    angle = 2.0 * np.pi * (np.arange(NZ)[:, None] * np.arange(NZ)[None, :] % NZ) / NZ
    c, s = np.cos(angle), np.sin(angle)
    if inverse:
        return halves(np.block([[c, -s], [s, c]]))
    return halves(FACTOR * np.block([[c, s], [-s, c]]))


def inverse_x_table():
    kx, x = np.arange(NX), np.arange(CROP)
    angle = 2.0 * np.pi * (kx[:, None] * x[None, :] % NX) / NX
    c, s = np.cos(angle), np.sin(angle)
    real = np.concatenate([c, s], axis=1).reshape(BLOCKS, LANES, 2 * CROP)
    imag = np.concatenate([-s, c], axis=1).reshape(BLOCKS, LANES, 2 * CROP)
    return halves(np.stack([real, imag], axis=1).reshape(2 * NX, 2 * CROP))


def inverse_y_table():
    group = np.arange(DEVICES)[:, None]
    j = np.arange(ROWS)[None, :]
    ky = 4 * group + np.where(group < DEVICES // 2, j, (4 - j) % 4)
    angle = 2.0 * np.pi * (np.arange(CROP)[:, None, None] * ky[None] % NY) / NY
    table = np.stack([np.cos(angle), -np.sin(angle)], axis=2)
    return halves(FACTOR * table.reshape(CROP, DEVICES * 8))


def split(a):
    high = a.astype(BF16)
    return high, (a - high.astype(F32)).astype(BF16)


def dot(a, b):
    return jnp.dot(a, b, preferred_element_type=F32)


def each(count, body, step):
    def several(i, carry):
        for at in range(step):
            body(step * i + at)
        return carry

    lax.fori_loop(0, count // step, several, 0)
    for k in range(count - count % step, count):
        body(k)


def kernel(
    frames_hbm, dy_hbm, cs_hbm, zf_hbm, zi_hbm, xi_hbm, yi_hbm, shifts_hbm, offsets_hbm, ref_hbm,
    corr, nout,
    frames, dy, cs, zf, zi, xi, yi, shifts, offsets,
    fhi, flo, sbuf, xbuf, rin, rbuf, cbuf, mbuf, nbuf, nrecv, ramp_xy, ramp_z,
    mine, abuf, g1hi, g1lo, gbuf, ybuf,
    send_x, recv_x, send_a, recv_a, send_n, recv_n, send_g, recv_g, ref_sem, own_sem,
    recv_y, first_sem, table_sem,
):
    g = lax.axis_index("grp")
    d = lax.axis_index("dev")
    me = 2 * d + g
    core, y_at, z_at = d % 2, (d // 2) % 4, (d // 8) % 4
    upper = d // 32

    barrier = pltpu.get_barrier_semaphore()

    early = [(frames_hbm, frames), (dy_hbm, dy), (cs_hbm, cs)]
    late = [(zf_hbm, zf), (zi_hbm, zi), (xi_hbm, xi), (yi_hbm, yi), (shifts_hbm, shifts), (offsets_hbm, offsets)]
    early = [pltpu.make_async_copy(a, b, first_sem.at[i]) for i, (a, b) in enumerate(early)]
    late = [pltpu.make_async_copy(a, b, table_sem.at[i]) for i, (a, b) in enumerate(late)]
    for copy in early:
        copy.start()

    def other(k):
        to = (me + 104 + k + jnp.where(k >= 24, 1, 0)) % DEVICES
        return to % 2, to // 2

    def greet(k):
        pl.semaphore_signal(barrier, 1, device_id=other(k), device_id_type=MESH)

    each(DEVICES - 1, greet, UNROLL)
    for copy in late:
        copy.start()
    for b in range(BLOCKS):
        pltpu.make_async_copy(ref_hbm.at[:, :, b * LANES : (b + 1) * LANES], rin.at[b], ref_sem).start()

    early[0].wait()
    for p in range(2):
        high, low = split(frames[p])
        fhi[p] = high
        flo[p] = low

    early[1].wait()
    early[2].wait()
    sub = lax.broadcasted_iota(jnp.int32, (1, 8, NX), 1)
    sigma = jnp.where(sub < 4, 1.0, -1.0).astype(F32)
    first = (sub % 4) == 0

    def send(chunk, k, which):
        half = (k + upper) % 2
        to_z = (z_at + k // 2) % 4
        to_y = jnp.where(half == 0, chunk + 8 - to_z, 10 - chunk - to_z) % 4
        within = 2 * ((core + k // 16) % 2) + (g + k // 8) % 2
        to = 64 * half + 16 * to_z + 4 * to_y + within
        slot = jnp.where(half == 0, GROUPS * chunk + 4 * to_z + within, 79 + GROUPS * chunk - 4 * to_z - within)
        blocks = slice(PASS, BLOCKS) if which else slice(0, PASS)
        source, target = sbuf.at[slot, blocks], xbuf.at[g, blocks, pl.ds(16 * d, 16)]

        @pl.when(to != me)
        def _():
            pltpu.make_async_remote_copy(
                source, target, send_x, recv_y if which else recv_x,
                device_id=(to % 2, to // 2), device_id_type=MESH,
            ).start()

        @pl.when(to == me)
        def _():
            pltpu.make_async_copy(source, target, own_sem).start()

    def forward(i, carry):
        chunk = (y_at + z_at + i) % CHUNKS
        base = pl.multiple_of(chunk * SPAN, 16)
        dyh = dy[0, pl.ds(base, SPAN), :]
        dyl = dy[1, pl.ds(base, SPAN), :]
        for p in range(2):
            rows = dot(dyh, fhi[p]) + dot(dyh, flo[p]) + dot(dyl, fhi[p])
            rh, rl = split(rows)
            prod = dot(rh, cs[0]) + dot(rl, cs[0]) + dot(rh, cs[1])
            prod = prod.reshape(GROUPS + 4, 8, 2 * NX)
            m1 = prod[:, :, :NX]
            t1 = sigma * pltpu.roll(prod[:, :, NX:], 4, 1)
            plus = (m1 + t1).reshape(4, 5, 8, NX)[:, :4].reshape(GROUPS, 8, NX)
            minus = (sigma * (m1 - t1)).reshape(4, 5, 8, NX)
            minus = jnp.where(first[None], minus[:, 1:], minus[:, :4]).reshape(GROUPS, 8, NX)
            for b in range(BLOCKS):
                lanes = slice(b * LANES, (b + 1) * LANES)
                sbuf[pl.ds(GROUPS * chunk, GROUPS), b, p * 8 : p * 8 + 8, :] = plus[:, :, lanes]
                sbuf[pl.ds(64 + GROUPS * chunk, GROUPS), b, p * 8 : p * 8 + 8, :] = minus[:, :, lanes]

        @pl.when(i == 0)
        def _():
            pl.semaphore_wait(barrier, DEVICES - 1)

        each(32, lambda k: send(chunk, k, 0), 4)
        return carry

    lax.fori_loop(0, CHUNKS, forward, 0)
    each(32 * CHUNKS, lambda k: send((y_at + z_at + k // 32) % CHUNKS, k % 32, 1), 4)

    def row_of(j):
        return jnp.where(upper == 0, j, (4 - j) % 4)

    for copy in late:
        copy.wait()
    pltpu.make_async_copy(rin, rin, ref_sem).wait()
    for part in range(2):
        for j in range(ROWS):
            for b in range(BLOCKS):
                rbuf[part, b, :, j * LANES : (j + 1) * LANES] = rin[
                    b, part, pl.ds(4 * g + row_of(j), NZ, stride=8), :
                ]

    lane = lax.broadcasted_iota(jnp.int32, (8, WIDE), 1)
    j_of = lane // LANES
    ky = 8 * d + 4 * g + jnp.where(upper == 0, j_of, (4 - j_of) % 4)
    kz = lax.broadcasted_iota(jnp.int32, (NZ, LANES), 0)
    unit = 2.0 * math.pi / NX
    for which, source in enumerate((shifts, offsets)):
        for t in range(2):
            sign = -1.0 if which == 0 else 1.0
            phase = (kz * source[t, 0]) % NZ
            angle = (4.0 * unit) * phase.astype(F32)
            ramp_z[which, t, 0] = jnp.cos(angle)
            ramp_z[which, t, 1] = sign * jnp.sin(angle)
            for b in range(BLOCKS):
                kx = b * LANES + lane % LANES
                phase = (ky * source[t, 1] + kx * source[t, 2]) % NX
                angle = unit * phase.astype(F32)
                ramp_xy[which, t, b, 0] = jnp.cos(angle)
                ramp_xy[which, t, b, 1] = sign * jnp.sin(angle)

    def turned(which, t, b, re, im):
        zr, zs = ramp_z[which, t, 0], ramp_z[which, t, 1]
        xr = ramp_xy[which, t, b, 0][:1]
        xs = ramp_xy[which, t, b, 1][:1]
        out_re, out_im = [], []
        for j in range(ROWS):
            lanes = slice(j * LANES, (j + 1) * LANES)
            ar, ai = xr[:, lanes], xs[:, lanes]
            cr = zr * ar - zs * ai
            ci = zr * ai + zs * ar
            out_re.append(re[:, lanes] * cr - im[:, lanes] * ci)
            out_im.append(re[:, lanes] * ci + im[:, lanes] * cr)
        return jnp.concatenate(out_re, axis=1), jnp.concatenate(out_im, axis=1)

    pltpu.make_async_copy(sbuf.at[0], sbuf.at[0], own_sem).wait()
    ahead, behind = sbuf.at[pl.ds(0, DEVICES - 1), 0:PASS], sbuf.at[pl.ds(0, DEVICES - 1), PASS:BLOCKS]
    pltpu.make_async_copy(ahead, ahead, recv_x).wait()

    half = NZ // 2

    def to_partner(b):
        return pltpu.make_async_remote_copy(
            nbuf.at[b, :, pl.ds((1 - g) * half, half)], nrecv.at[b], send_n, recv_n,
            device_id=(1 - g, d), device_id_type=MESH,
        )

    def spectrum(b, sums):
        @pl.when(b == PASS)
        def _():
            pltpu.make_async_copy(behind, behind, recv_y).wait()

        zh, zl = zf[0], zf[1]
        ref_re, ref_im = rbuf[0, b], rbuf[1, b]
        new_re, new_im = 0.5 * ref_re, 0.5 * ref_im
        found = []
        for t in range(2):
            re = [xbuf[t, b, pl.ds(j, NZ, stride=8), :] for j in range(ROWS)]
            im = [xbuf[t, b, pl.ds(4 + j, NZ, stride=8), :] for j in range(ROWS)]
            both = jnp.concatenate([jnp.concatenate(re, axis=1), jnp.concatenate(im, axis=1)], axis=0)
            bh, bl = split(both)
            freq = dot(zh, bh) + dot(zl, bh) + dot(zh, bl)
            fr, fi = freq[:NZ], freq[NZ:]
            cross_re = fr * ref_re + fi * ref_im
            cross_im = fi * ref_re - fr * ref_im
            magnitude = jnp.sqrt(cross_re * cross_re + cross_im * cross_im)
            cbuf[t, b, :NZ] = cross_re
            cbuf[t, b, NZ:] = cross_im
            mbuf[t, b] = magnitude
            found.append(sums[t] + magnitude.reshape(NZ // 8, 8, WIDE).sum(axis=0))
            wr, wi = turned(0, t, b, fr, fi)
            new_re += 0.25 * wr
            new_im += 0.25 * wi
        nbuf[b, 0] = new_re
        nbuf[b, 1] = new_im

        @pl.when(b < EARLY)
        def _():
            to_partner(b).start()

        return tuple(found)

    sums = lax.fori_loop(0, BLOCKS, spectrum, (jnp.zeros((8, WIDE), F32),) * 2)

    lane1 = lax.broadcasted_iota(jnp.int32, (1, LANES), 1)
    mine[...] = jnp.where(lane1 < 64, jnp.sum(sums[0]), jnp.sum(sums[1]))

    def tell(k):
        pltpu.make_async_remote_copy(
            mine, abuf.at[me], send_a, recv_a, device_id=other(k), device_id_type=MESH
        ).start()

    each(DEVICES - 1, tell, UNROLL)
    pltpu.make_async_copy(mine, abuf.at[me], own_sem).start()

    for b in range(EARLY, BLOCKS):
        to_partner(b).start()

    def keep(source, at_grp):
        for b in range(BLOCKS):
            for part in range(2):
                for j in range(ROWS):
                    nout[part, pl.ds(8 * b + 4 * at_grp + row_of(j), half, stride=8 * BLOCKS), :] = source[
                        b, part, :, j * LANES : (j + 1) * LANES
                    ]

    keep(nbuf.at[:, :, pl.ds(g * half, half)], g)

    def turn(b, carry):
        for t in range(2):
            cbuf[t, b, :NZ], cbuf[t, b, NZ:] = turned(1, t, b, cbuf[t, b, :NZ], cbuf[t, b, NZ:])
        return carry

    lax.fori_loop(0, BLOCKS, turn, 0)

    pltpu.make_async_copy(mine, abuf.at[me], own_sem).wait()
    pltpu.make_async_copy(abuf.at[pl.ds(0, DEVICES - 1)], abuf.at[pl.ds(0, DEVICES - 1)], recv_a).wait()
    total = jnp.sum(abuf[...].reshape(DEVICES, LANES), axis=0, keepdims=True) / (NZ * NY * NX)

    def back(i, carry):
        t = (g + i) % 2
        average = jnp.sum(jnp.where(lane1 == 64 * t, total, 0.0))

        def whiten(b, inner):
            zh, zl = zi[0], zi[1]
            scale = 1.0 / (mbuf[t, b] + average)
            both = cbuf[t, b] * jnp.concatenate([scale, scale], axis=0)
            bh, bl = split(both)
            depth = dot(zh, bh) + dot(zl, bh) + dot(zh, bl)
            dh, dl = split(depth)
            for part in range(2):
                for j in range(ROWS):
                    at = pl.ds(pl.multiple_of((2 * b + part) * LANES, LANES), LANES)
                    rows = slice(part * NZ, (part + 1) * NZ)
                    lanes = slice(j * LANES, (j + 1) * LANES)
                    g1hi[j * NZ : (j + 1) * NZ, at] = dh[rows, lanes]
                    g1lo[j * NZ : (j + 1) * NZ, at] = dl[rows, lanes]
            return inner

        lax.fori_loop(0, BLOCKS, whiten, 0)
        width = dot(g1hi[...], xi[0]) + dot(g1lo[...], xi[0]) + dot(g1hi[...], xi[1])
        for part in range(2):
            for j in range(ROWS):
                gbuf[t, pl.ds(4 * part + j, NZ, stride=8), :] = width[
                    j * NZ : (j + 1) * NZ, part * CROP : (part + 1) * CROP
                ]

        def send_back(k):
            to = (d + k) % 64

            @pl.when((to != d) | (t != g))
            def _():
                pltpu.make_async_remote_copy(
                    gbuf.at[t, pl.ds(16 * to, 16)], ybuf.at[me], send_g, recv_g,
                    device_id=(t, to), device_id_type=MESH,
                ).start()

            @pl.when((to == d) & (t == g))
            def _():
                pltpu.make_async_copy(gbuf.at[t, pl.ds(16 * to, 16)], ybuf.at[me], own_sem).start()

        each(64, send_back, 4)
        return carry

    lax.fori_loop(0, 2, back, 0)

    pltpu.make_async_copy(nrecv, nrecv, recv_n).wait()
    keep(nrecv, 1 - g)

    pltpu.make_async_copy(ybuf.at[0], ybuf.at[0], own_sem).wait()
    pltpu.make_async_copy(ybuf.at[pl.ds(0, DEVICES - 1)], ybuf.at[pl.ds(0, DEVICES - 1)], recv_g).wait()
    for p in range(2):
        rows = ybuf[:, p * 8 : p * 8 + 8, :].reshape(DEVICES * 8, CROP)
        rh, rl = split(rows)
        corr[p] = dot(yi[0], rh) + dot(yi[1], rh) + dot(yi[0], rl)

    pltpu.make_async_copy(sbuf.at[pl.ds(0, DEVICES - 1)], sbuf.at[pl.ds(0, DEVICES - 1)], send_x).wait()
    pltpu.make_async_copy(abuf.at[pl.ds(0, DEVICES - 1)], abuf.at[pl.ds(0, DEVICES - 1)], send_a).wait()
    pltpu.make_async_copy(ybuf.at[pl.ds(0, DEVICES - 1)], ybuf.at[pl.ds(0, DEVICES - 1)], send_g).wait()
    pltpu.make_async_copy(nrecv, nrecv, send_n).wait()


def local(frames, ref_spectrum, shifts, offsets):
    vmem = pl.BlockSpec(memory_space=pltpu.VMEM)
    hbm = pl.BlockSpec(memory_space=pltpu.HBM)
    corr, new = pl.pallas_call(
        kernel,
        out_shape=(
            jax.ShapeDtypeStruct((2, CROP, CROP), F32),
            jax.ShapeDtypeStruct((2, NZ // 2 * BLOCKS * 8, LANES), F32),
        ),
        in_specs=[hbm] * 10,
        out_specs=(vmem, vmem),
        scratch_shapes=[
            pltpu.VMEM((2, NY, NX), F32),
            pltpu.VMEM((2, CHUNKS * SPAN, NY), BF16),
            pltpu.VMEM((2, NX, 2 * NX), BF16),
            pltpu.VMEM((2, 2 * NZ, 2 * NZ), BF16),
            pltpu.VMEM((2, 2 * NZ, 2 * NZ), BF16),
            pltpu.VMEM((2, 2 * NX, 2 * CROP), BF16),
            pltpu.VMEM((2, CROP, DEVICES * 8), BF16),
            pltpu.SMEM((2, 3), jnp.int32),
            pltpu.SMEM((2, 3), jnp.int32),
            pltpu.VMEM((2, NY, NX), BF16),
            pltpu.VMEM((2, NY, NX), BF16),
            pltpu.VMEM((DEVICES, BLOCKS, 16, LANES), F32),
            pltpu.VMEM((2, BLOCKS, NZ * 8, LANES), F32),
            pltpu.VMEM((BLOCKS, 2, NZ * 8, LANES), F32),
            pltpu.VMEM((2, BLOCKS, NZ, WIDE), F32),
            pltpu.VMEM((2, BLOCKS, 2 * NZ, WIDE), F32),
            pltpu.VMEM((2, BLOCKS, NZ, WIDE), F32),
            pltpu.VMEM((BLOCKS, 2, NZ, WIDE), F32),
            pltpu.VMEM((BLOCKS, 2, NZ // 2, WIDE), F32),
            pltpu.VMEM((2, 2, BLOCKS, 2, 8, WIDE), F32),
            pltpu.VMEM((2, 2, 2, NZ, LANES), F32),
            pltpu.VMEM((1, LANES), F32),
            pltpu.VMEM((DEVICES, 1, LANES), F32),
            pltpu.VMEM((ROWS * NZ, 2 * NX), BF16),
            pltpu.VMEM((ROWS * NZ, 2 * NX), BF16),
            pltpu.VMEM((2, NZ * 8, LANES), F32),
            pltpu.VMEM((DEVICES, 16, LANES), F32),
        ]
        + [pltpu.SemaphoreType.DMA] * 11
        + [pltpu.SemaphoreType.DMA((3,)), pltpu.SemaphoreType.DMA((6,))],
        compiler_params=pltpu.CompilerParams(
            collective_id=0, has_side_effects=True, vmem_limit_bytes=46 << 20
        ),
    )(
        *(
            pltpu.with_memory_space_constraint(x, pltpu.HBM)
            for x in (
                frames[0],
                jnp.asarray(forward_y_table()),
                jnp.asarray(forward_x_table()),
                jnp.asarray(z_table(False)),
                jnp.asarray(z_table(True)),
                jnp.asarray(inverse_x_table()),
                jnp.asarray(inverse_y_table()),
                shifts,
                offsets,
                ref_spectrum.reshape(2, NZ * 8, NX),
            )
        )
    )
    new = new.reshape(2, NZ // 2, BLOCKS, 8, LANES).transpose(0, 1, 3, 2, 4)
    return corr[None], new.reshape(2, NZ // 2, 8, NX)


def solution(mesh):
    return jax.shard_map(
        local,
        mesh=mesh,
        in_specs=(P("grp", "dev", None, None), P(None, None, "dev", None), P(), P()),
        out_specs=(P("grp", "dev", None, None), P(None, "grp", "dev", None)),
        check_vma=False,
    )
```

```python
import math

import jax
import jax.numpy as jnp
import numpy as np
from jax import lax
from jax.experimental import pallas as pl
from jax.experimental.pallas import tpu as pltpu
from jax.sharding import PartitionSpec as P

NX = 512
NY = 512
NZ = 128
CROP = 128
ROWS = 4
LANES = 128
BLOCKS = NX // LANES
WIDE = ROWS * LANES
DEVICES = 128
CHUNKS = 4
GROUPS = 16
SPAN = (GROUPS + 4) * 8
FACTOR = 1.0 / math.sqrt(NZ * NY * NX)
F32 = jnp.float32
BF16 = jnp.bfloat16
MESH = pl.DeviceIdType.MESH
UNROLL = 8
EARLY = 2
PASS = 2


def halves(table):
    single = table.astype(np.float32)
    high = single.astype(jnp.bfloat16)
    low = (table - high.astype(np.float64)).astype(np.float32).astype(jnp.bfloat16)
    return np.stack([high, low])


def forward_y_table():
    out = np.zeros((CHUNKS, 4, 5, 2, ROWS, NY))
    y = np.arange(NY)
    for chunk in range(CHUNKS):
        for run in range(4):
            for at in range(5):
                for j in range(ROWS):
                    ky = 4 * (16 * run + 4 * ((chunk - run) % 4) + at) + j
                    angle = 2.0 * np.pi * (ky * y % NY) / NY
                    out[chunk, run, at, 0, j] = np.cos(angle)
                    out[chunk, run, at, 1, j] = -np.sin(angle)
    return halves(out.reshape(CHUNKS * SPAN, NY))


def forward_x_table():
    angle = 2.0 * np.pi * (np.arange(NX)[:, None] * np.arange(NX)[None, :] % NX) / NX
    return halves(np.concatenate([np.cos(angle), np.sin(angle)], axis=1))


def z_table(inverse):
    angle = 2.0 * np.pi * (np.arange(NZ)[:, None] * np.arange(NZ)[None, :] % NZ) / NZ
    c, s = np.cos(angle), np.sin(angle)
    if inverse:
        return halves(np.block([[c, -s], [s, c]]))
    return halves(FACTOR * np.block([[c, s], [-s, c]]))


def inverse_x_table():
    kx, x = np.arange(NX), np.arange(CROP)
    angle = 2.0 * np.pi * (kx[:, None] * x[None, :] % NX) / NX
    c, s = np.cos(angle), np.sin(angle)
    real = np.concatenate([c, s], axis=1).reshape(BLOCKS, LANES, 2 * CROP)
    imag = np.concatenate([-s, c], axis=1).reshape(BLOCKS, LANES, 2 * CROP)
    return halves(np.stack([real, imag], axis=1).reshape(2 * NX, 2 * CROP))


def inverse_y_table():
    group = np.arange(DEVICES)[:, None]
    j = np.arange(ROWS)[None, :]
    ky = 4 * group + np.where(group < DEVICES // 2, j, (4 - j) % 4)
    angle = 2.0 * np.pi * (np.arange(CROP)[:, None, None] * ky[None] % NY) / NY
    table = np.stack([np.cos(angle), -np.sin(angle)], axis=2)
    return halves(FACTOR * table.reshape(CROP, DEVICES * 8))


def split(a):
    high = a.astype(BF16)
    return high, (a - high.astype(F32)).astype(BF16)


def dot(a, b):
    return jnp.dot(a, b, preferred_element_type=F32)


def each(count, body, step):
    def several(i, carry):
        for at in range(step):
            body(step * i + at)
        return carry

    lax.fori_loop(0, count // step, several, 0)
    for k in range(count - count % step, count):
        body(k)


def kernel(
    frames_hbm, dy_hbm, cs_hbm, zf_hbm, zi_hbm, xi_hbm, yi_hbm, shifts_hbm, offsets_hbm, ref_hbm,
    ybuf, nout, yi,
    frames, dy, cs, zf, zi, xi, shifts, offsets,
    fhi, flo, sbuf, xbuf, rin, rbuf, cbuf, mbuf, nbuf, nrecv, ramp_xy, ramp_z,
    mine, abuf, g1hi, g1lo, gbuf,
    send_x, recv_x, send_a, recv_a, send_n, recv_n, send_g, recv_g, ref_sem, own_sem,
    recv_y, first_sem, table_sem,
):
    g = lax.axis_index("grp")
    d = lax.axis_index("dev")
    me = 2 * d + g
    core, y_at, z_at = d % 2, (d // 2) % 4, (d // 8) % 4
    upper = d // 32

    barrier = pltpu.get_barrier_semaphore()

    early = [(frames_hbm, frames), (dy_hbm, dy), (cs_hbm, cs)]
    late = [(zf_hbm, zf), (zi_hbm, zi), (xi_hbm, xi), (yi_hbm, yi), (shifts_hbm, shifts), (offsets_hbm, offsets)]
    early = [pltpu.make_async_copy(a, b, first_sem.at[i]) for i, (a, b) in enumerate(early)]
    late = [pltpu.make_async_copy(a, b, table_sem.at[i]) for i, (a, b) in enumerate(late)]
    for copy in early:
        copy.start()

    def other(k):
        to = (me + 104 + k + jnp.where(k >= 24, 1, 0)) % DEVICES
        return to % 2, to // 2

    def greet(k):
        pl.semaphore_signal(barrier, 1, device_id=other(k), device_id_type=MESH)

    each(DEVICES - 1, greet, UNROLL)
    for copy in late:
        copy.start()
    for b in range(BLOCKS):
        pltpu.make_async_copy(ref_hbm.at[:, :, b * LANES : (b + 1) * LANES], rin.at[b], ref_sem).start()

    early[0].wait()
    for p in range(2):
        high, low = split(frames[p])
        fhi[p] = high
        flo[p] = low

    early[1].wait()
    early[2].wait()
    sub = lax.broadcasted_iota(jnp.int32, (1, 8, NX), 1)
    sigma = jnp.where(sub < 4, 1.0, -1.0).astype(F32)
    first = (sub % 4) == 0

    def send(chunk, k, which):
        half = (k + upper) % 2
        to_z = (z_at + k // 2) % 4
        to_y = jnp.where(half == 0, chunk + 8 - to_z, 10 - chunk - to_z) % 4
        within = 2 * ((core + k // 16) % 2) + (g + k // 8) % 2
        to = 64 * half + 16 * to_z + 4 * to_y + within
        slot = jnp.where(half == 0, GROUPS * chunk + 4 * to_z + within, 79 + GROUPS * chunk - 4 * to_z - within)
        blocks = slice(PASS, BLOCKS) if which else slice(0, PASS)
        source, target = sbuf.at[slot, blocks], xbuf.at[g, blocks, pl.ds(16 * d, 16)]

        @pl.when(to != me)
        def _():
            pltpu.make_async_remote_copy(
                source, target, send_x, recv_y if which else recv_x,
                device_id=(to % 2, to // 2), device_id_type=MESH,
            ).start()

        @pl.when(to == me)
        def _():
            pltpu.make_async_copy(source, target, own_sem).start()

    def forward(i, carry):
        chunk = (y_at + z_at + i) % CHUNKS
        base = pl.multiple_of(chunk * SPAN, 16)
        dyh = dy[0, pl.ds(base, SPAN), :]
        dyl = dy[1, pl.ds(base, SPAN), :]
        for p in range(2):
            rows = dot(dyh, fhi[p]) + dot(dyh, flo[p]) + dot(dyl, fhi[p])
            rh, rl = split(rows)
            prod = dot(rh, cs[0]) + dot(rl, cs[0]) + dot(rh, cs[1])
            prod = prod.reshape(GROUPS + 4, 8, 2 * NX)
            m1 = prod[:, :, :NX]
            t1 = sigma * pltpu.roll(prod[:, :, NX:], 4, 1)
            plus = (m1 + t1).reshape(4, 5, 8, NX)[:, :4].reshape(GROUPS, 8, NX)
            minus = (sigma * (m1 - t1)).reshape(4, 5, 8, NX)
            minus = jnp.where(first[None], minus[:, 1:], minus[:, :4]).reshape(GROUPS, 8, NX)
            for b in range(BLOCKS):
                lanes = slice(b * LANES, (b + 1) * LANES)
                sbuf[pl.ds(GROUPS * chunk, GROUPS), b, p * 8 : p * 8 + 8, :] = plus[:, :, lanes]
                sbuf[pl.ds(64 + GROUPS * chunk, GROUPS), b, p * 8 : p * 8 + 8, :] = minus[:, :, lanes]

        @pl.when(i == 0)
        def _():
            pl.semaphore_wait(barrier, DEVICES - 1)

        each(32, lambda k: send(chunk, k, 0), 4)
        return carry

    lax.fori_loop(0, CHUNKS, forward, 0)
    each(32 * CHUNKS, lambda k: send((y_at + z_at + k // 32) % CHUNKS, k % 32, 1), 4)

    def row_of(j):
        return jnp.where(upper == 0, j, (4 - j) % 4)

    for copy in late:
        copy.wait()
    pltpu.make_async_copy(rin, rin, ref_sem).wait()
    for part in range(2):
        for j in range(ROWS):
            for b in range(BLOCKS):
                rbuf[part, b, :, j * LANES : (j + 1) * LANES] = rin[
                    b, part, pl.ds(4 * g + row_of(j), NZ, stride=8), :
                ]

    lane = lax.broadcasted_iota(jnp.int32, (8, WIDE), 1)
    j_of = lane // LANES
    ky = 8 * d + 4 * g + jnp.where(upper == 0, j_of, (4 - j_of) % 4)
    kz = lax.broadcasted_iota(jnp.int32, (NZ, LANES), 0)
    unit = 2.0 * math.pi / NX
    for which, source in enumerate((shifts, offsets)):
        for t in range(2):
            sign = -1.0 if which == 0 else 1.0
            phase = (kz * source[t, 0]) % NZ
            angle = (4.0 * unit) * phase.astype(F32)
            ramp_z[which, t, 0] = jnp.cos(angle)
            ramp_z[which, t, 1] = sign * jnp.sin(angle)
            for b in range(BLOCKS):
                kx = b * LANES + lane % LANES
                phase = (ky * source[t, 1] + kx * source[t, 2]) % NX
                angle = unit * phase.astype(F32)
                ramp_xy[which, t, b, 0] = jnp.cos(angle)
                ramp_xy[which, t, b, 1] = sign * jnp.sin(angle)

    def turned(which, t, b, re, im):
        zr, zs = ramp_z[which, t, 0], ramp_z[which, t, 1]
        xr = ramp_xy[which, t, b, 0][:1]
        xs = ramp_xy[which, t, b, 1][:1]
        out_re, out_im = [], []
        for j in range(ROWS):
            lanes = slice(j * LANES, (j + 1) * LANES)
            ar, ai = xr[:, lanes], xs[:, lanes]
            cr = zr * ar - zs * ai
            ci = zr * ai + zs * ar
            out_re.append(re[:, lanes] * cr - im[:, lanes] * ci)
            out_im.append(re[:, lanes] * ci + im[:, lanes] * cr)
        return jnp.concatenate(out_re, axis=1), jnp.concatenate(out_im, axis=1)

    pltpu.make_async_copy(sbuf.at[0], sbuf.at[0], own_sem).wait()
    ahead, behind = sbuf.at[pl.ds(0, DEVICES - 1), 0:PASS], sbuf.at[pl.ds(0, DEVICES - 1), PASS:BLOCKS]
    pltpu.make_async_copy(ahead, ahead, recv_x).wait()

    half = NZ // 2

    def to_partner(b):
        return pltpu.make_async_remote_copy(
            nbuf.at[b, :, pl.ds((1 - g) * half, half)], nrecv.at[b], send_n, recv_n,
            device_id=(1 - g, d), device_id_type=MESH,
        )

    def spectrum(b, sums):
        @pl.when(b == PASS)
        def _():
            pltpu.make_async_copy(behind, behind, recv_y).wait()

        zh, zl = zf[0], zf[1]
        ref_re, ref_im = rbuf[0, b], rbuf[1, b]
        new_re, new_im = 0.5 * ref_re, 0.5 * ref_im
        found = []
        for t in range(2):
            re = [xbuf[t, b, pl.ds(j, NZ, stride=8), :] for j in range(ROWS)]
            im = [xbuf[t, b, pl.ds(4 + j, NZ, stride=8), :] for j in range(ROWS)]
            both = jnp.concatenate([jnp.concatenate(re, axis=1), jnp.concatenate(im, axis=1)], axis=0)
            bh, bl = split(both)
            freq = dot(zh, bh) + dot(zl, bh) + dot(zh, bl)
            fr, fi = freq[:NZ], freq[NZ:]
            cross_re = fr * ref_re + fi * ref_im
            cross_im = fi * ref_re - fr * ref_im
            magnitude = jnp.sqrt(cross_re * cross_re + cross_im * cross_im)
            cbuf[t, b, :NZ] = cross_re
            cbuf[t, b, NZ:] = cross_im
            mbuf[t, b] = magnitude
            found.append(sums[t] + magnitude.reshape(NZ // 8, 8, WIDE).sum(axis=0))
            wr, wi = turned(0, t, b, fr, fi)
            new_re += 0.25 * wr
            new_im += 0.25 * wi
        nbuf[b, 0] = new_re
        nbuf[b, 1] = new_im

        @pl.when(b < EARLY)
        def _():
            to_partner(b).start()

        return tuple(found)

    sums = lax.fori_loop(0, BLOCKS, spectrum, (jnp.zeros((8, WIDE), F32),) * 2)

    lane1 = lax.broadcasted_iota(jnp.int32, (1, LANES), 1)
    mine[...] = jnp.where(lane1 < 64, jnp.sum(sums[0]), jnp.sum(sums[1]))

    def tell(k):
        pltpu.make_async_remote_copy(
            mine, abuf.at[me], send_a, recv_a, device_id=other(k), device_id_type=MESH
        ).start()

    each(DEVICES - 1, tell, UNROLL)
    pltpu.make_async_copy(mine, abuf.at[me], own_sem).start()

    for b in range(EARLY, BLOCKS):
        to_partner(b).start()

    def keep(source, at_grp):
        for b in range(BLOCKS):
            for part in range(2):
                for j in range(ROWS):
                    nout[part, pl.ds(8 * b + 4 * at_grp + row_of(j), half, stride=8 * BLOCKS), :] = source[
                        b, part, :, j * LANES : (j + 1) * LANES
                    ]

    keep(nbuf.at[:, :, pl.ds(g * half, half)], g)

    def turn(b, carry):
        for t in range(2):
            cbuf[t, b, :NZ], cbuf[t, b, NZ:] = turned(1, t, b, cbuf[t, b, :NZ], cbuf[t, b, NZ:])
        return carry

    lax.fori_loop(0, BLOCKS, turn, 0)

    pltpu.make_async_copy(mine, abuf.at[me], own_sem).wait()
    pltpu.make_async_copy(abuf.at[pl.ds(0, DEVICES - 1)], abuf.at[pl.ds(0, DEVICES - 1)], recv_a).wait()
    total = jnp.sum(abuf[...].reshape(DEVICES, LANES), axis=0, keepdims=True) / (NZ * NY * NX)

    def back(i, carry):
        t = (g + i) % 2
        average = jnp.sum(jnp.where(lane1 == 64 * t, total, 0.0))

        def whiten(b, inner):
            zh, zl = zi[0], zi[1]
            scale = 1.0 / (mbuf[t, b] + average)
            both = cbuf[t, b] * jnp.concatenate([scale, scale], axis=0)
            bh, bl = split(both)
            depth = dot(zh, bh) + dot(zl, bh) + dot(zh, bl)
            dh, dl = split(depth)
            for part in range(2):
                for j in range(ROWS):
                    at = pl.ds(pl.multiple_of((2 * b + part) * LANES, LANES), LANES)
                    rows = slice(part * NZ, (part + 1) * NZ)
                    lanes = slice(j * LANES, (j + 1) * LANES)
                    g1hi[j * NZ : (j + 1) * NZ, at] = dh[rows, lanes]
                    g1lo[j * NZ : (j + 1) * NZ, at] = dl[rows, lanes]
            return inner

        lax.fori_loop(0, BLOCKS, whiten, 0)
        width = dot(g1hi[...], xi[0]) + dot(g1lo[...], xi[0]) + dot(g1hi[...], xi[1])
        for part in range(2):
            for j in range(ROWS):
                gbuf[t, pl.ds(4 * part + j, NZ, stride=8), :] = width[
                    j * NZ : (j + 1) * NZ, part * CROP : (part + 1) * CROP
                ]

        def send_back(k):
            to = (d + k) % 64

            @pl.when((to != d) | (t != g))
            def _():
                pltpu.make_async_remote_copy(
                    gbuf.at[t, pl.ds(16 * to, 16)], ybuf.at[me], send_g, recv_g,
                    device_id=(t, to), device_id_type=MESH,
                ).start()

            @pl.when((to == d) & (t == g))
            def _():
                pltpu.make_async_copy(gbuf.at[t, pl.ds(16 * to, 16)], ybuf.at[me], own_sem).start()

        each(64, send_back, 4)
        return carry

    lax.fori_loop(0, 2, back, 0)

    pltpu.make_async_copy(nrecv, nrecv, recv_n).wait()
    keep(nrecv, 1 - g)

    pltpu.make_async_copy(ybuf.at[0], ybuf.at[0], own_sem).wait()
    pltpu.make_async_copy(ybuf.at[pl.ds(0, DEVICES - 1)], ybuf.at[pl.ds(0, DEVICES - 1)], recv_g).wait()
    pltpu.make_async_copy(sbuf.at[pl.ds(0, DEVICES - 1)], sbuf.at[pl.ds(0, DEVICES - 1)], send_x).wait()
    pltpu.make_async_copy(abuf.at[pl.ds(0, DEVICES - 1)], abuf.at[pl.ds(0, DEVICES - 1)], send_a).wait()
    pltpu.make_async_copy(ybuf.at[pl.ds(0, DEVICES - 1)], ybuf.at[pl.ds(0, DEVICES - 1)], send_g).wait()
    pltpu.make_async_copy(nrecv, nrecv, send_n).wait()


def finish(ybuf, rows, yi, corr, out, sem):
    copy = pltpu.make_async_copy(rows, out, sem)
    copy.start()
    for p in range(2):
        high, low = split(ybuf[:, p * 8 : p * 8 + 8, :].reshape(DEVICES * 8, CROP))
        corr[p] = dot(yi[0], high) + dot(yi[1], high) + dot(yi[0], low)
    copy.wait()


def local(frames, ref_spectrum, shifts, offsets):
    vmem = pl.BlockSpec(memory_space=pltpu.VMEM)
    hbm = pl.BlockSpec(memory_space=pltpu.HBM)
    planes, rows, table = pl.pallas_call(
        kernel,
        out_shape=(
            jax.ShapeDtypeStruct((DEVICES, 16, LANES), F32),
            jax.ShapeDtypeStruct((2, NZ // 2 * BLOCKS * 8, LANES), F32),
            jax.ShapeDtypeStruct((2, CROP, DEVICES * 8), BF16),
        ),
        in_specs=[hbm] * 10,
        out_specs=(vmem, vmem, vmem),
        scratch_shapes=[
            pltpu.VMEM((2, NY, NX), F32),
            pltpu.VMEM((2, CHUNKS * SPAN, NY), BF16),
            pltpu.VMEM((2, NX, 2 * NX), BF16),
            pltpu.VMEM((2, 2 * NZ, 2 * NZ), BF16),
            pltpu.VMEM((2, 2 * NZ, 2 * NZ), BF16),
            pltpu.VMEM((2, 2 * NX, 2 * CROP), BF16),
            pltpu.SMEM((2, 3), jnp.int32),
            pltpu.SMEM((2, 3), jnp.int32),
            pltpu.VMEM((2, NY, NX), BF16),
            pltpu.VMEM((2, NY, NX), BF16),
            pltpu.VMEM((DEVICES, BLOCKS, 16, LANES), F32),
            pltpu.VMEM((2, BLOCKS, NZ * 8, LANES), F32),
            pltpu.VMEM((BLOCKS, 2, NZ * 8, LANES), F32),
            pltpu.VMEM((2, BLOCKS, NZ, WIDE), F32),
            pltpu.VMEM((2, BLOCKS, 2 * NZ, WIDE), F32),
            pltpu.VMEM((2, BLOCKS, NZ, WIDE), F32),
            pltpu.VMEM((BLOCKS, 2, NZ, WIDE), F32),
            pltpu.VMEM((BLOCKS, 2, NZ // 2, WIDE), F32),
            pltpu.VMEM((2, 2, BLOCKS, 2, 8, WIDE), F32),
            pltpu.VMEM((2, 2, 2, NZ, LANES), F32),
            pltpu.VMEM((1, LANES), F32),
            pltpu.VMEM((DEVICES, 1, LANES), F32),
            pltpu.VMEM((ROWS * NZ, 2 * NX), BF16),
            pltpu.VMEM((ROWS * NZ, 2 * NX), BF16),
            pltpu.VMEM((2, NZ * 8, LANES), F32),
        ]
        + [pltpu.SemaphoreType.DMA] * 11
        + [pltpu.SemaphoreType.DMA((3,)), pltpu.SemaphoreType.DMA((6,))],
        compiler_params=pltpu.CompilerParams(
            collective_id=0, has_side_effects=True, vmem_limit_bytes=46 << 20
        ),
    )(
        *(
            pltpu.with_memory_space_constraint(x, pltpu.HBM)
            for x in (
                frames[0],
                jnp.asarray(forward_y_table()),
                jnp.asarray(forward_x_table()),
                jnp.asarray(z_table(False)),
                jnp.asarray(z_table(True)),
                jnp.asarray(inverse_x_table()),
                jnp.asarray(inverse_y_table()),
                shifts,
                offsets,
                ref_spectrum.reshape(2, NZ * 8, NX),
            )
        )
    )
    corr, new = pl.pallas_call(
        finish,
        out_shape=(
            jax.ShapeDtypeStruct((2, CROP, CROP), F32),
            jax.ShapeDtypeStruct(rows.shape, F32),
        ),
        in_specs=[vmem] * 3,
        out_specs=(vmem, hbm),
        scratch_shapes=[pltpu.SemaphoreType.DMA],
        compiler_params=pltpu.CompilerParams(vmem_limit_bytes=16 << 20),
    )(planes, rows, table)
    new = new.reshape(2, NZ // 2, BLOCKS, 8, LANES).transpose(0, 1, 3, 2, 4)
    return corr[None], new.reshape(2, NZ // 2, 8, NX)


def solution(mesh):
    return jax.shard_map(
        local,
        mesh=mesh,
        in_specs=(P("grp", "dev", None, None), P(None, None, "dev", None), P(), P()),
        out_specs=(P("grp", "dev", None, None), P(None, "grp", "dev", None)),
        check_vma=False,
    )
```

```python
import math

import jax
import jax.numpy as jnp
import numpy as np
from jax import lax
from jax.experimental import pallas as pl
from jax.experimental.pallas import tpu as pltpu
from jax.sharding import PartitionSpec as P

NX = 512
NY = 512
NZ = 128
CROP = 128
ROWS = 4
LANES = 128
BLOCKS = NX // LANES
WIDE = ROWS * LANES
DEVICES = 128
CHUNKS = 4
GROUPS = 16
SPAN = (GROUPS + 4) * 8
FACTOR = 1.0 / math.sqrt(NZ * NY * NX)
F32 = jnp.float32
BF16 = jnp.bfloat16
MESH = pl.DeviceIdType.MESH
UNROLL = 8
EARLY = 2
PASS = 2


def halves(table):
    single = table.astype(np.float32)
    high = single.astype(jnp.bfloat16)
    low = (table - high.astype(np.float64)).astype(np.float32).astype(jnp.bfloat16)
    return np.stack([high, low])


def forward_y_table():
    out = np.zeros((CHUNKS, 4, 5, 2, ROWS, NY))
    y = np.arange(NY)
    for chunk in range(CHUNKS):
        for run in range(4):
            for at in range(5):
                for j in range(ROWS):
                    ky = 4 * (16 * run + 4 * ((chunk - run) % 4) + at) + j
                    angle = 2.0 * np.pi * (ky * y % NY) / NY
                    out[chunk, run, at, 0, j] = np.cos(angle)
                    out[chunk, run, at, 1, j] = -np.sin(angle)
    return halves(out.reshape(CHUNKS * SPAN, NY))


def forward_x_table():
    angle = 2.0 * np.pi * (np.arange(NX)[:, None] * np.arange(NX)[None, :] % NX) / NX
    return halves(np.concatenate([np.cos(angle), np.sin(angle)], axis=1))


def z_table(inverse):
    angle = 2.0 * np.pi * (np.arange(NZ)[:, None] * np.arange(NZ)[None, :] % NZ) / NZ
    c, s = np.cos(angle), np.sin(angle)
    if inverse:
        return halves(np.block([[c, -s], [s, c]]))
    return halves(FACTOR * np.block([[c, s], [-s, c]]))


def inverse_x_table():
    kx, x = np.arange(NX), np.arange(CROP)
    angle = 2.0 * np.pi * (kx[:, None] * x[None, :] % NX) / NX
    c, s = np.cos(angle), np.sin(angle)
    real = np.concatenate([c, s], axis=1).reshape(BLOCKS, LANES, 2 * CROP)
    imag = np.concatenate([-s, c], axis=1).reshape(BLOCKS, LANES, 2 * CROP)
    return halves(np.stack([real, imag], axis=1).reshape(2 * NX, 2 * CROP))


def inverse_y_table():
    group = np.arange(DEVICES)[:, None]
    j = np.arange(ROWS)[None, :]
    ky = 4 * group + np.where(group < DEVICES // 2, j, (4 - j) % 4)
    angle = 2.0 * np.pi * (np.arange(CROP)[:, None, None] * ky[None] % NY) / NY
    table = np.stack([np.cos(angle), -np.sin(angle)], axis=2)
    return halves(FACTOR * table.reshape(CROP, DEVICES * 8))


def split(a):
    high = a.astype(BF16)
    return high, (a - high.astype(F32)).astype(BF16)


def dot(a, b):
    return jnp.dot(a, b, preferred_element_type=F32)


def each(count, body, step):
    def several(i, carry):
        for at in range(step):
            body(step * i + at)
        return carry

    lax.fori_loop(0, count // step, several, 0)
    for k in range(count - count % step, count):
        body(k)


def kernel(
    frames_hbm, dy_hbm, cs_hbm, zf_hbm, zi_hbm, xi_hbm, yi_hbm, shifts_hbm, offsets_hbm, ref_hbm,
    ybuf, nout, yi,
    frames, dy, cs, zf, zi, xi, shifts, offsets,
    fhi, flo, sbuf, xbuf, rin, rbuf, cbuf, mbuf, nbuf, nrecv, ramp_xy, ramp_z,
    mine, abuf, g1hi, g1lo, gbuf,
    send_x, recv_x, send_a, recv_a, send_n, recv_n, send_g, recv_g, ref_sem, own_sem,
    recv_y, first_sem, table_sem,
):
    g = lax.axis_index("grp")
    d = lax.axis_index("dev")
    me = 2 * d + g
    core, y_at, z_at = d % 2, (d // 2) % 4, (d // 8) % 4
    upper = d // 32

    barrier = pltpu.get_barrier_semaphore()

    early = [(frames_hbm, frames), (dy_hbm, dy), (cs_hbm, cs)]
    late = [(zf_hbm, zf), (zi_hbm, zi), (xi_hbm, xi), (yi_hbm, yi), (shifts_hbm, shifts), (offsets_hbm, offsets)]
    early = [pltpu.make_async_copy(a, b, first_sem.at[i]) for i, (a, b) in enumerate(early)]
    late = [pltpu.make_async_copy(a, b, table_sem.at[i]) for i, (a, b) in enumerate(late)]
    for copy in early:
        copy.start()

    def other(k):
        to = (me + 104 + k + jnp.where(k >= 24, 1, 0)) % DEVICES
        return to % 2, to // 2

    def greet(k):
        pl.semaphore_signal(barrier, 1, device_id=other(k), device_id_type=MESH)

    each(DEVICES - 1, greet, 16)
    for copy in late:
        copy.start()
    for b in range(BLOCKS):
        pltpu.make_async_copy(ref_hbm.at[:, :, b * LANES : (b + 1) * LANES], rin.at[b], ref_sem).start()

    early[0].wait()
    for p in range(2):
        high, low = split(frames[p])
        fhi[p] = high
        flo[p] = low

    early[1].wait()
    early[2].wait()
    sub = lax.broadcasted_iota(jnp.int32, (1, 8, NX), 1)
    sigma = jnp.where(sub < 4, 1.0, -1.0).astype(F32)
    first = (sub % 4) == 0

    def send(chunk, k, which):
        half = (k + upper) % 2
        to_z = (z_at + k // 2) % 4
        to_y = jnp.where(half == 0, chunk + 8 - to_z, 10 - chunk - to_z) % 4
        within = 2 * ((core + k // 16) % 2) + (g + k // 8) % 2
        to = 64 * half + 16 * to_z + 4 * to_y + within
        slot = jnp.where(half == 0, GROUPS * chunk + 4 * to_z + within, 79 + GROUPS * chunk - 4 * to_z - within)
        blocks = slice(PASS, BLOCKS) if which else slice(0, PASS)
        source, target = sbuf.at[slot, blocks], xbuf.at[g, blocks, pl.ds(16 * d, 16)]

        @pl.when(to != me)
        def _():
            pltpu.make_async_remote_copy(
                source, target, send_x, recv_y if which else recv_x,
                device_id=(to % 2, to // 2), device_id_type=MESH,
            ).start()

        @pl.when(to == me)
        def _():
            pltpu.make_async_copy(source, target, own_sem).start()

    def forward(i, carry):
        chunk = (y_at + z_at + i) % CHUNKS
        base = pl.multiple_of(chunk * SPAN, 16)
        dyh = dy[0, pl.ds(base, SPAN), :]
        dyl = dy[1, pl.ds(base, SPAN), :]
        for p in range(2):
            rows = dot(dyh, fhi[p]) + dot(dyh, flo[p]) + dot(dyl, fhi[p])
            rh, rl = split(rows)
            prod = dot(rh, cs[0]) + dot(rl, cs[0]) + dot(rh, cs[1])
            prod = prod.reshape(GROUPS + 4, 8, 2 * NX)
            m1 = prod[:, :, :NX]
            t1 = sigma * pltpu.roll(prod[:, :, NX:], 4, 1)
            plus = (m1 + t1).reshape(4, 5, 8, NX)[:, :4].reshape(GROUPS, 8, NX)
            minus = (sigma * (m1 - t1)).reshape(4, 5, 8, NX)
            minus = jnp.where(first[None], minus[:, 1:], minus[:, :4]).reshape(GROUPS, 8, NX)
            for b in range(BLOCKS):
                lanes = slice(b * LANES, (b + 1) * LANES)
                sbuf[pl.ds(GROUPS * chunk, GROUPS), b, p * 8 : p * 8 + 8, :] = plus[:, :, lanes]
                sbuf[pl.ds(64 + GROUPS * chunk, GROUPS), b, p * 8 : p * 8 + 8, :] = minus[:, :, lanes]

        @pl.when(i == 0)
        def _():
            pl.semaphore_wait(barrier, DEVICES - 1)

        each(32, lambda k: send(chunk, k, 0), 4)
        return carry

    lax.fori_loop(0, CHUNKS, forward, 0)
    each(32 * CHUNKS, lambda k: send((y_at + z_at + k // 32) % CHUNKS, k % 32, 1), 4)

    def row_of(j):
        return jnp.where(upper == 0, j, (4 - j) % 4)

    for copy in late:
        copy.wait()
    pltpu.make_async_copy(rin, rin, ref_sem).wait()
    for part in range(2):
        for j in range(ROWS):
            for b in range(BLOCKS):
                rbuf[part, b, :, j * LANES : (j + 1) * LANES] = rin[
                    b, part, pl.ds(4 * g + row_of(j), NZ, stride=8), :
                ]

    lane = lax.broadcasted_iota(jnp.int32, (8, WIDE), 1)
    j_of = lane // LANES
    ky = 8 * d + 4 * g + jnp.where(upper == 0, j_of, (4 - j_of) % 4)
    kz = lax.broadcasted_iota(jnp.int32, (NZ, LANES), 0)
    unit = 2.0 * math.pi / NX
    for which, source in enumerate((shifts, offsets)):
        for t in range(2):
            sign = -1.0 if which == 0 else 1.0
            phase = (kz * source[t, 0]) % NZ
            angle = (4.0 * unit) * phase.astype(F32)
            ramp_z[which, t, 0] = jnp.cos(angle)
            ramp_z[which, t, 1] = sign * jnp.sin(angle)
            for b in range(BLOCKS):
                kx = b * LANES + lane % LANES
                phase = (ky * source[t, 1] + kx * source[t, 2]) % NX
                angle = unit * phase.astype(F32)
                ramp_xy[which, t, b, 0] = jnp.cos(angle)
                ramp_xy[which, t, b, 1] = sign * jnp.sin(angle)

    def turned(which, t, b, re, im):
        zr, zs = ramp_z[which, t, 0], ramp_z[which, t, 1]
        xr = ramp_xy[which, t, b, 0][:1]
        xs = ramp_xy[which, t, b, 1][:1]
        out_re, out_im = [], []
        for j in range(ROWS):
            lanes = slice(j * LANES, (j + 1) * LANES)
            ar, ai = xr[:, lanes], xs[:, lanes]
            cr = zr * ar - zs * ai
            ci = zr * ai + zs * ar
            out_re.append(re[:, lanes] * cr - im[:, lanes] * ci)
            out_im.append(re[:, lanes] * ci + im[:, lanes] * cr)
        return jnp.concatenate(out_re, axis=1), jnp.concatenate(out_im, axis=1)

    pltpu.make_async_copy(sbuf.at[0], sbuf.at[0], own_sem).wait()
    ahead, behind = sbuf.at[pl.ds(0, DEVICES - 1), 0:PASS], sbuf.at[pl.ds(0, DEVICES - 1), PASS:BLOCKS]
    pltpu.make_async_copy(ahead, ahead, recv_x).wait()

    half = NZ // 2

    def to_partner(b):
        return pltpu.make_async_remote_copy(
            nbuf.at[b, :, pl.ds((1 - g) * half, half)], nrecv.at[b], send_n, recv_n,
            device_id=(1 - g, d), device_id_type=MESH,
        )

    def spectrum(b, sums):
        @pl.when(b == PASS)
        def _():
            pltpu.make_async_copy(behind, behind, recv_y).wait()

        zh, zl = zf[0], zf[1]
        ref_re, ref_im = rbuf[0, b], rbuf[1, b]
        new_re, new_im = 0.5 * ref_re, 0.5 * ref_im
        found = []
        for t in range(2):
            re = [xbuf[t, b, pl.ds(j, NZ, stride=8), :] for j in range(ROWS)]
            im = [xbuf[t, b, pl.ds(4 + j, NZ, stride=8), :] for j in range(ROWS)]
            both = jnp.concatenate([jnp.concatenate(re, axis=1), jnp.concatenate(im, axis=1)], axis=0)
            bh, bl = split(both)
            freq = dot(zh, bh) + dot(zl, bh) + dot(zh, bl)
            fr, fi = freq[:NZ], freq[NZ:]
            cross_re = fr * ref_re + fi * ref_im
            cross_im = fi * ref_re - fr * ref_im
            magnitude = jnp.sqrt(cross_re * cross_re + cross_im * cross_im)
            cbuf[t, b, :NZ] = cross_re
            cbuf[t, b, NZ:] = cross_im
            mbuf[t, b] = magnitude
            found.append(sums[t] + magnitude.reshape(NZ // 8, 8, WIDE).sum(axis=0))
            wr, wi = turned(0, t, b, fr, fi)
            new_re += 0.25 * wr
            new_im += 0.25 * wi
        nbuf[b, 0] = new_re
        nbuf[b, 1] = new_im

        @pl.when(b < EARLY)
        def _():
            to_partner(b).start()

        return tuple(found)

    sums = lax.fori_loop(0, BLOCKS, spectrum, (jnp.zeros((8, WIDE), F32),) * 2)

    lane1 = lax.broadcasted_iota(jnp.int32, (1, LANES), 1)
    mine[...] = jnp.where(lane1 < 64, jnp.sum(sums[0]), jnp.sum(sums[1]))

    def tell(k):
        pltpu.make_async_remote_copy(
            mine, abuf.at[me], send_a, recv_a, device_id=other(k), device_id_type=MESH
        ).start()

    each(DEVICES - 1, tell, UNROLL)
    pltpu.make_async_copy(mine, abuf.at[me], own_sem).start()

    for b in range(EARLY, BLOCKS):
        to_partner(b).start()

    def keep(source, at_grp):
        for b in range(BLOCKS):
            for part in range(2):
                for j in range(ROWS):
                    nout[part, pl.ds(8 * b + 4 * at_grp + row_of(j), half, stride=8 * BLOCKS), :] = source[
                        b, part, :, j * LANES : (j + 1) * LANES
                    ]

    keep(nbuf.at[:, :, pl.ds(g * half, half)], g)

    def turn(b, carry):
        for t in range(2):
            cbuf[t, b, :NZ], cbuf[t, b, NZ:] = turned(1, t, b, cbuf[t, b, :NZ], cbuf[t, b, NZ:])
        return carry

    lax.fori_loop(0, BLOCKS, turn, 0)

    pltpu.make_async_copy(mine, abuf.at[me], own_sem).wait()
    pltpu.make_async_copy(abuf.at[pl.ds(0, DEVICES - 1)], abuf.at[pl.ds(0, DEVICES - 1)], recv_a).wait()
    total = jnp.sum(abuf[...].reshape(DEVICES, LANES), axis=0, keepdims=True) / (NZ * NY * NX)

    def back(i, carry):
        t = (g + i) % 2
        average = jnp.sum(jnp.where(lane1 == 64 * t, total, 0.0))

        def whiten(b, inner):
            zh, zl = zi[0], zi[1]
            scale = 1.0 / (mbuf[t, b] + average)
            both = cbuf[t, b] * jnp.concatenate([scale, scale], axis=0)
            bh, bl = split(both)
            depth = dot(zh, bh) + dot(zl, bh) + dot(zh, bl)
            dh, dl = split(depth)
            for part in range(2):
                for j in range(ROWS):
                    at = pl.ds(pl.multiple_of((2 * b + part) * LANES, LANES), LANES)
                    rows = slice(part * NZ, (part + 1) * NZ)
                    lanes = slice(j * LANES, (j + 1) * LANES)
                    g1hi[j * NZ : (j + 1) * NZ, at] = dh[rows, lanes]
                    g1lo[j * NZ : (j + 1) * NZ, at] = dl[rows, lanes]
            return inner

        lax.fori_loop(0, BLOCKS, whiten, 0)
        width = dot(g1hi[...], xi[0]) + dot(g1lo[...], xi[0]) + dot(g1hi[...], xi[1])
        for part in range(2):
            for j in range(ROWS):
                gbuf[t, pl.ds(4 * part + j, NZ, stride=8), :] = width[
                    j * NZ : (j + 1) * NZ, part * CROP : (part + 1) * CROP
                ]

        def send_back(k):
            to = (d + k) % 64

            @pl.when((to != d) | (t != g))
            def _():
                pltpu.make_async_remote_copy(
                    gbuf.at[t, pl.ds(16 * to, 16)], ybuf.at[me], send_g, recv_g,
                    device_id=(t, to), device_id_type=MESH,
                ).start()

            @pl.when((to == d) & (t == g))
            def _():
                pltpu.make_async_copy(gbuf.at[t, pl.ds(16 * to, 16)], ybuf.at[me], own_sem).start()

        each(64, send_back, 4)
        return carry

    lax.fori_loop(0, 2, back, 0)

    pltpu.make_async_copy(nrecv, nrecv, recv_n).wait()
    keep(nrecv, 1 - g)

    pltpu.make_async_copy(ybuf.at[0], ybuf.at[0], own_sem).wait()
    pltpu.make_async_copy(ybuf.at[pl.ds(0, DEVICES - 1)], ybuf.at[pl.ds(0, DEVICES - 1)], recv_g).wait()
    pltpu.make_async_copy(sbuf.at[pl.ds(0, DEVICES - 1)], sbuf.at[pl.ds(0, DEVICES - 1)], send_x).wait()
    pltpu.make_async_copy(abuf.at[pl.ds(0, DEVICES - 1)], abuf.at[pl.ds(0, DEVICES - 1)], send_a).wait()
    pltpu.make_async_copy(ybuf.at[pl.ds(0, DEVICES - 1)], ybuf.at[pl.ds(0, DEVICES - 1)], send_g).wait()
    pltpu.make_async_copy(nrecv, nrecv, send_n).wait()


def finish(ybuf, rows, yi, corr, out, sem):
    copy = pltpu.make_async_copy(rows, out, sem)
    copy.start()
    planes = [ybuf[:, p * 8 : p * 8 + 8, :].reshape(DEVICES * 8, CROP) for p in range(2)]
    high, low = split(jnp.concatenate(planes, axis=1))
    both = dot(yi[0], high) + dot(yi[1], high) + dot(yi[0], low)
    for p in range(2):
        corr[p] = both[:, p * CROP : (p + 1) * CROP]
    copy.wait()


def local(frames, ref_spectrum, shifts, offsets):
    vmem = pl.BlockSpec(memory_space=pltpu.VMEM)
    hbm = pl.BlockSpec(memory_space=pltpu.HBM)
    planes, rows, table = pl.pallas_call(
        kernel,
        out_shape=(
            jax.ShapeDtypeStruct((DEVICES, 16, LANES), F32),
            jax.ShapeDtypeStruct((2, NZ // 2 * BLOCKS * 8, LANES), F32),
            jax.ShapeDtypeStruct((2, CROP, DEVICES * 8), BF16),
        ),
        in_specs=[hbm] * 10,
        out_specs=(vmem, vmem, vmem),
        scratch_shapes=[
            pltpu.VMEM((2, NY, NX), F32),
            pltpu.VMEM((2, CHUNKS * SPAN, NY), BF16),
            pltpu.VMEM((2, NX, 2 * NX), BF16),
            pltpu.VMEM((2, 2 * NZ, 2 * NZ), BF16),
            pltpu.VMEM((2, 2 * NZ, 2 * NZ), BF16),
            pltpu.VMEM((2, 2 * NX, 2 * CROP), BF16),
            pltpu.SMEM((2, 3), jnp.int32),
            pltpu.SMEM((2, 3), jnp.int32),
            pltpu.VMEM((2, NY, NX), BF16),
            pltpu.VMEM((2, NY, NX), BF16),
            pltpu.VMEM((DEVICES, BLOCKS, 16, LANES), F32),
            pltpu.VMEM((2, BLOCKS, NZ * 8, LANES), F32),
            pltpu.VMEM((BLOCKS, 2, NZ * 8, LANES), F32),
            pltpu.VMEM((2, BLOCKS, NZ, WIDE), F32),
            pltpu.VMEM((2, BLOCKS, 2 * NZ, WIDE), F32),
            pltpu.VMEM((2, BLOCKS, NZ, WIDE), F32),
            pltpu.VMEM((BLOCKS, 2, NZ, WIDE), F32),
            pltpu.VMEM((BLOCKS, 2, NZ // 2, WIDE), F32),
            pltpu.VMEM((2, 2, BLOCKS, 2, 8, WIDE), F32),
            pltpu.VMEM((2, 2, 2, NZ, LANES), F32),
            pltpu.VMEM((1, LANES), F32),
            pltpu.VMEM((DEVICES, 1, LANES), F32),
            pltpu.VMEM((ROWS * NZ, 2 * NX), BF16),
            pltpu.VMEM((ROWS * NZ, 2 * NX), BF16),
            pltpu.VMEM((2, NZ * 8, LANES), F32),
        ]
        + [pltpu.SemaphoreType.DMA] * 11
        + [pltpu.SemaphoreType.DMA((3,)), pltpu.SemaphoreType.DMA((6,))],
        compiler_params=pltpu.CompilerParams(
            collective_id=0, has_side_effects=True, vmem_limit_bytes=46 << 20
        ),
    )(
        *(
            pltpu.with_memory_space_constraint(x, pltpu.HBM)
            for x in (
                frames[0],
                jnp.asarray(forward_y_table()),
                jnp.asarray(forward_x_table()),
                jnp.asarray(z_table(False)),
                jnp.asarray(z_table(True)),
                jnp.asarray(inverse_x_table()),
                jnp.asarray(inverse_y_table()),
                shifts,
                offsets,
                ref_spectrum.reshape(2, NZ * 8, NX),
            )
        )
    )
    corr, new = pl.pallas_call(
        finish,
        out_shape=(
            jax.ShapeDtypeStruct((2, CROP, CROP), F32),
            jax.ShapeDtypeStruct(rows.shape, F32),
        ),
        in_specs=[vmem] * 3,
        out_specs=(vmem, hbm),
        scratch_shapes=[pltpu.SemaphoreType.DMA],
        compiler_params=pltpu.CompilerParams(vmem_limit_bytes=16 << 20),
    )(planes, rows, table)
    new = new.reshape(2, NZ // 2, BLOCKS, 8, LANES).transpose(0, 1, 3, 2, 4)
    return corr[None], new.reshape(2, NZ // 2, 8, NX)


def solution(mesh):
    return jax.shard_map(
        local,
        mesh=mesh,
        in_specs=(P("grp", "dev", None, None), P(None, None, "dev", None), P(), P()),
        out_specs=(P("grp", "dev", None, None), P(None, "grp", "dev", None)),
        check_vma=False,
    )
```
